512 devices in a mesh: state: 8 (over y_lo, x), bond: 64 (over z, y_hi, core).
Axes of the slice: x: 4, y: 8 (y_hi: 4, y_lo: 2; y = y_hi * 2 + y_lo), z: 8, core: 2. Of those that a mesh axis runs over, the one named last changes fastest.
Arguments:
- intersect_left: bfloat16 [8, 2048, 2048], P('state', 'bond'), may hold values from -0.125 to 0.125
- stored_block: bfloat16 [8, 4, 2048, 2048], P('state', None, 'bond'), may hold values from -6 to 6
- stored_site: bfloat16 [8, 2, 2048, 2048], P('state', None, 'bond'), may hold values from -6 to 6
- current_site: bfloat16 [2048, 2, 2048], P('bond', None, 'state'), may hold values from -0.09375 to 0.09375
- current_block: bfloat16 [4, 2048, 2048], P(None, 'bond', 'state'), may hold values from -6 to 6
- penalty_weight: float32 [8], replicated, may hold values from 0.5 to 4
Outputs:
- penalized: float32 [4, 2048, 2048], P(None, 'bond', 'state')
- intersect_next: bfloat16 [8, 2048, 2048], P('state', 'bond')
The draws below stay inside these ranges and needn't reach their ends.
All inputs are finite; a program needn't handle non-finite values.
Results may differ from the reference program's by a relative error of at most 0.0055.
Values may be sent and summed in bfloat16 or wider, within the bound.
A program may use at most 64 MiB of HBM per device.

```python
import math
import jax
import jax.numpy as jnp

D = 2048
PHYS = 2
Q = 4
STATES = 8


def level_of(rng, dims, pieces, least, high):
    def one(axis_at, shards_of):
        draws = jax.random.uniform(jax.random.fold_in(jax.random.fold_in(rng, 6), axis_at), (shards_of,), jnp.float32, least / len(pieces), high / len(pieces))
        return jnp.repeat(jnp.exp(draws), dims[axis_at] // shards_of).reshape((-1,) + (1,) * (len(dims) - axis_at - 1))

    factor_of = one(*pieces[0])
    for cut in pieces[1:]:
        factor_of = factor_of * one(*cut)
    return factor_of


def normal_values(key, dims, scale, limit, split=(), kind=jnp.bfloat16):
    result = scale * jax.random.normal(key, dims, jnp.float32)
    if split:
        result = result * level_of(key, dims, split, -0.22, 0.18)
    return jnp.clip(result, -limit, limit).astype(kind)


def setup_inputs(seed: int = 0) -> dict:
    seeds = jax.random.split(jax.random.key(seed), 7)
    return {
        "intersect_left": normal_values(seeds[0], (STATES, D, D), D ** -0.5, 0.125, ((0, 8), (1, 64))),
        "stored_block": normal_values(seeds[1], (STATES, Q, D, D), 1.0, 6.0, ((0, 8), (2, 64))),
        "stored_site": normal_values(seeds[2], (STATES, PHYS, D, D), 1.0, 6.0, ((0, 8), (2, 64))),
        "current_site": normal_values(seeds[3], (D, PHYS, D), (PHYS * D) ** -0.5, 0.09375, ((0, 64), (2, 8))),
        "current_block": normal_values(seeds[4], (Q, D, D), 1.0, 6.0, ((1, 64), (2, 8))),
        "penalty_weight": jnp.clip(jnp.exp(jax.random.uniform(seeds[5], (STATES,), jnp.float32, math.log(0.5), math.log(4.0))), 0.5, 4.0),
    }


def reference(intersect_left, stored_block, stored_site, current_site, current_block, penalty_weight):
    block_wide = current_block.astype(jnp.float32)
    site_wide = current_site.astype(jnp.float32)
    penalized = block_wide
    grown_list = []
    for index in range(STATES):
        env_turned = intersect_left[index].T
        projected = jnp.dot(stored_block[index].reshape(Q * D, D), env_turned, preferred_element_type=jnp.float32).reshape(Q, D, D)
        intersect = jnp.sum(projected * block_wide) / (PHYS * D)
        penalized = penalized + (penalty_weight[index] * intersect) * projected
        moved = jnp.dot(stored_site[index].reshape(PHYS * D, D), env_turned, preferred_element_type=jnp.float32).astype(jnp.bfloat16)
        moved = moved.reshape(PHYS, D, D).astype(jnp.float32)
        grown = jnp.einsum("asf,sea->fe", site_wide, moved).astype(jnp.bfloat16)
        grown_list.append(grown)
    return penalized, jnp.stack(grown_list)
```

```python
import functools

import jax
import jax.numpy as jnp
from jax import lax
from jax.experimental import pallas as pl
from jax.experimental.pallas import tpu as pltpu
from jax.sharding import Mesh
from jax.sharding import PartitionSpec as P

BF = jnp.bfloat16
F32 = jnp.float32
STATE = ("yl", "x")
BOND = ("z", "yh", "c")
TURN = (0, 1, 3, 2)
WIDE = 2048
SITE = 512
COLS = WIDE + SITE

COMMON = [
    (0, 0), (1, 0), (0, 1), (0, 2), (2, 0), (0, 3),
    (1, 1), (1, 2), (1, 3), (2, 1), (2, 2), (2, 3),
]
UP_ORDER = COMMON + [(3, 0), (3, 1), (3, 2), (3, 3)]
DOWN_ORDER = COMMON + [(3, 2), (3, 3), (3, 0), (3, 1)]


def slot_up(s):
    return 0 if s == 0 else (7 if s == 4 else 2 * s - 1)


def slot_down(s):
    return 0 if s == 0 else (7 if s == 4 else 2 * s)


def remote(src, dst, send, recv, device):
    return pltpu.make_async_remote_copy(
        src_ref=src, dst_ref=dst, send_sem=send, recv_sem=recv,
        device_id=device, device_id_type=pl.DeviceIdType.MESH,
    )


def lanes_to_halves(low, high):
    lane = lax.broadcasted_iota(jnp.int32, low.shape, 1) // 32
    first = jnp.where(lane == 0, low, jnp.where(lane == 1, pltpu.roll(low, 96, 1),
                      jnp.where(lane == 2, pltpu.roll(high, 64, 1), pltpu.roll(high, 32, 1))))
    second = jnp.where(lane == 0, pltpu.roll(low, 96, 1), jnp.where(lane == 1, pltpu.roll(low, 64, 1),
                       jnp.where(lane == 2, pltpu.roll(high, 32, 1), high)))
    return first, second


def halves_to_lanes(first, second):
    lane = lax.broadcasted_iota(jnp.int32, first.shape, 1) // 32
    low = jnp.where(lane == 0, first, jnp.where(lane == 1, pltpu.roll(second, 32, 1),
                    jnp.where(lane == 2, pltpu.roll(first, 32, 1), pltpu.roll(second, 64, 1))))
    high = jnp.where(lane == 0, pltpu.roll(first, 64, 1), jnp.where(lane == 1, pltpu.roll(second, 96, 1),
                     jnp.where(lane == 2, pltpu.roll(first, 96, 1), second)))
    return low, high


def kernel(chunk_ref, block_ref, site_ref, current_ref, weight_ref, pen_ref, next_ref,
           rows, stored, proj_out, proj_in, moved, grown, grown_in, tiles_out, tiles_in, dots,
           local_sem, y_send, y_recv, z_send, z_recv, s_send, s_recv, p_send, p_recv,
           m_send, m_recv, g_send, g_recv, o_send, o_recv, r_send, r_recv):
    yl, x, z, yh, c = (lax.axis_index(n) for n in ("yl", "x", "z", "yh", "c"))
    state = yl * 4 + x
    up = {"z": lax.rem(z + 1, 8)}
    down = {"z": lax.rem(z + 7, 8)}
    sibling = {"c": 1 - c}
    partner = {"yl": 1 - yl}

    def source(q):
        return lax.rem(yh + TURN[q], 4)

    mine = pltpu.make_async_copy(chunk_ref, rows.at[0, yh], local_sem.at[0])
    mine.start()
    own = [
        pltpu.make_async_copy(block_ref.at[0], stored.at[pl.ds(0, 4), c], local_sem.at[1]),
        pltpu.make_async_copy(site_ref.at[0], stored.at[pl.ds(4, 2), c], local_sem.at[2]),
    ]
    for copy in own:
        copy.start()
    swap = [
        remote(block_ref.at[0], stored.at[pl.ds(0, 4), c], s_send.at[0], s_recv.at[0], sibling),
        remote(site_ref.at[0], stored.at[pl.ds(4, 2), c], s_send.at[1], s_recv.at[1], sibling),
    ]
    mine.wait()

    def pass_up(s, q):
        block = source(q)
        return remote(rows.at[slot_up(s), block], rows.at[slot_up(s + 1), block],
                      z_send, z_recv.at[0, s + 1, q], up)

    def pass_down(s, q):
        block = source(q)
        return remote(rows.at[slot_down(s), block], rows.at[slot_down(s + 1), block],
                      z_send, z_recv.at[1, s + 1, q], down)

    def give(q):
        return remote(rows.at[0, yh], rows.at[0, yh], y_send, y_recv.at[q],
                      {"yh": lax.rem(yh + 4 - TURN[q], 4)})

    pass_up(0, 0).start()
    pass_down(0, 0).start()
    for q in (1, 2, 3):
        give(q).start()
    for copy in swap:
        copy.start()

    low, high = (current_ref[:, :, 128 * h:128 * (h + 1)].astype(F32).reshape(128, 128) for h in (0, 1))
    current = lanes_to_halves(low, high)

    for copy in own:
        copy.wait()
    for copy in swap:
        copy.wait_recv()
    grown[...] = jnp.zeros_like(grown)

    def row_of(t):
        if t == 7:
            return lax.rem(z + 4, 8)
        d = (t + 1) // 2
        return lax.rem(z + (8 - d if t % 2 else d), 8)

    def to_state(t, same):
        r = row_of(t)
        core = c if same else 1 - c
        return remote(proj_out.at[t, core], proj_in.at[state, c], p_send, p_recv.at[state, c],
                      {"yl": r // 4, "x": lax.rem(r, 4), "c": core})

    def moved_copy(t, other, device, sem):
        k = (1 - yl if other else yl) * 4 + x
        return remote(moved.at[t, k], moved.at[t, k], m_send, m_recv.at[t, sem], device)

    def along_x(t, other):
        return [moved_copy(t, other, {"x": lax.rem(x + o, 4)}, (4 if other else 0) + o) for o in (1, 2, 3)]

    def multiply(t):
        left = stored[...].reshape(384, WIDE)
        right = rows[t, :, :, 0:WIDE].reshape(128, WIDE)
        product = lax.dot_general(left, right, (((1,), (1,)), ((), ())), preferred_element_type=F32).astype(BF)
        blocks = product[0:256].reshape(4, 2, 32, 128)
        for j in (0, 1):
            proj_out[t, j] = blocks[:, j].reshape(128, 128)
        moved[t, state] = product[256:384]
        moved_copy(t, False, partner, 4).start()
        for copy in along_x(t, False):
            copy.start()
        home = row_of(t) == state

        @pl.when(home)
        def _():
            proj_in[state, c] = proj_out[t, c]

        @pl.when(jnp.logical_not(home))
        def _():
            to_state(t, True).start()

        to_state(t, False).start()

    def relay(t):
        moved_copy(t, False, partner, 4).wait_recv()
        for copy in along_x(t, True):
            copy.start()

    def grow(t):
        for other in (False, True):
            for copy in along_x(t, other):
                copy.wait_recv()
        for s in (0, 1):
            site = rows[t, :, :, WIDE + 256 * s:WIDE + 256 * (s + 1)].reshape(128, 256)
            right = moved[t, :, 64 * s:64 * (s + 1), :].reshape(512, 128)
            grown[...] += lax.dot_general(site, right, (((0,), (1,)), ((), ())), preferred_element_type=F32)

    done = []

    def step(t):
        multiply(t)
        done.append(t)
        if len(done) >= 2:
            relay(done[-2])
        if len(done) >= 4:
            grow(done[-4])

    for place in range(16):
        for order, passing, lane, last in ((UP_ORDER, pass_up, 0, (0, 1)), (DOWN_ORDER, pass_down, 1, (2, 3))):
            s, q = order[place]
            if s == 0:
                if lane == 0 and q > 0:
                    give(q).wait_recv()
            else:
                passing(s - 1, q).wait_recv()
            if (s, q) != (0, 0) and (s < 3 or q in last):
                passing(s, q).start()
        s, q = UP_ORDER[place]
        if q == 3:
            if s == 0:
                step(0)
            else:
                step(slot_up(s))
                step(slot_down(s))
    for q in (0, 1):
        pass_up(3, q).wait_recv()
    for q in (2, 3):
        pass_down(3, q).wait_recv()
    multiply(7)
    relay(6)
    relay(7)
    for t in done[-3:]:
        grow(t)

    for k in range(8):
        for i in (0, 1):
            @pl.when(jnp.logical_or(k != state, i != c))
            def _():
                pltpu.make_async_copy(proj_in.at[k, i], proj_in.at[k, i], p_recv.at[k, i]).wait()
    partial = [
        sum(jnp.sum((proj_in[k, i].astype(F32) * current[i]).reshape(16, 8, 128), axis=0) for i in (0, 1))
        for k in range(8)
    ]
    partial = jnp.concatenate([jnp.sum(p, axis=0, keepdims=True) for p in partial], axis=0)

    places = (x * 2 + c, z, yl * 4 + yh)

    def peer(stage, o):
        there = lax.rem(places[stage] + o, 8)
        if stage == 0:
            return {"x": there // 2, "c": lax.rem(there, 2)}
        if stage == 1:
            return {"z": there}
        return {"yl": there // 4, "yh": lax.rem(there, 4)}

    def exchange(stage, value):
        dots[stage, places[stage]] = value
        for o in range(1, 8):
            here = dots.at[stage, places[stage]]
            remote(here, here, r_send.at[stage], r_recv.at[stage], peer(stage, o)).start()

    def collected(stage):
        seven = dots.at[stage, pl.ds(0, 7)]
        pltpu.make_async_copy(seven, seven, r_recv.at[stage]).wait()
        return jnp.sum(dots[stage], axis=0)

    exchange(0, partial)
    grow(7)
    give_half = remote(grown.at[pl.ds(128 * (1 - c), 128)], grown_in, g_send, g_recv, sibling)
    give_half.start()
    exchange(1, collected(0))
    give_half.wait_recv()

    lane = lax.broadcasted_iota(jnp.int32, (16, 128), 1)
    half = grown.at[pl.ds(pl.multiple_of(128 * c, 128), 128)]
    for d in range(4):
        for pair in range(4):
            cut = pl.ds(128 * pair, 128)
            first = half[pl.ds(32 * d, 16), cut] + grown_in[pl.ds(32 * d, 16), cut]
            second = half[pl.ds(32 * d + 16, 16), cut] + grown_in[pl.ds(32 * d + 16, 16), cut]
            tiles_out[2 * pair, d] = jnp.where(lane < 64, first, pltpu.roll(second, 64, 1)).astype(BF)
            tiles_out[2 * pair + 1, d] = jnp.where(lane < 64, pltpu.roll(first, 64, 1), second).astype(BF)

    place = z * 4 + yh
    for k in range(8):
        for d in range(4):
            to = 2 * c + d // 2
            here = jnp.logical_and(jnp.logical_and(k == state, z == state), jnp.logical_and(to == yh, d % 2 == c))

            @pl.when(here)
            def _():
                pltpu.make_async_copy(tiles_out.at[k, d], tiles_in.at[place], o_recv).start()

            @pl.when(jnp.logical_not(here))
            def _():
                remote(tiles_out.at[k, d], tiles_in.at[place], o_send, o_recv,
                       {"yl": k // 4, "x": k % 4, "z": state, "yh": to, "c": d % 2}).start()

    exchange(2, collected(1))
    total = jnp.sum(collected(2), axis=1, keepdims=True) * (1.0 / 4096.0)
    factor = total * weight_ref[...]
    halves = []
    for i in (0, 1):
        value = current[i]
        for k in range(8):
            value = value + factor[k:k + 1, :] * proj_in[k, i].astype(F32)
        halves.append(value)
    low, high = halves_to_lanes(*halves)
    pen_ref[:, :, 0:128] = low.reshape(4, 32, 128)
    pen_ref[:, :, 128:256] = high.reshape(4, 32, 128)

    pltpu.make_async_copy(tiles_in, tiles_in, o_recv).wait()
    for p in range(16):
        even = tiles_in[2 * p].astype(F32)
        odd = tiles_in[2 * p + 1].astype(F32)
        cut = slice(128 * p, 128 * (p + 1))
        next_ref[0, 0:16, cut] = jnp.where(lane < 64, even, pltpu.roll(odd, 64, 1)).astype(BF)
        next_ref[0, 16:32, cut] = jnp.where(lane < 64, pltpu.roll(even, 64, 1), odd).astype(BF)

    def drained(ref, sem):
        pltpu.make_async_copy(ref, ref, sem).wait()

    for copy in swap:
        copy.wait_send()
    drained(rows.at[0, pl.ds(0, 3)], y_send)
    drained(rows.at[pl.ds(0, 7)], z_send)
    drained(proj_in.at[pl.ds(0, 7)], p_send)
    drained(proj_in.at[0, 0], p_send)
    drained(moved.at[pl.ds(0, 7)], m_send)
    give_half.wait_send()
    for stage in range(3):
        drained(dots.at[stage, pl.ds(0, 7)], r_send.at[stage])
    drained(tiles_in.at[pl.ds(0, 31)], o_send)

    @pl.when(jnp.logical_not(jnp.logical_and(z == state, yh // 2 == c)))
    def _():
        drained(tiles_in.at[0], o_send)


def shards(intersect_left, stored_block, stored_site, current_site, current_block, penalty_weight):
    chunk = jnp.concatenate([intersect_left[0], current_site.reshape(32, SITE)], axis=1)
    weight = jnp.broadcast_to(penalty_weight[:, None], (8, 128))
    hbm = pl.BlockSpec(memory_space=pl.ANY)
    vmem = pl.BlockSpec(memory_space=pltpu.VMEM)
    dma = pltpu.SemaphoreType.DMA
    return pl.pallas_call(
        kernel,
        out_shape=(
            jax.ShapeDtypeStruct((4, 32, 256), F32),
            jax.ShapeDtypeStruct((1, 32, 2048), BF),
        ),
        in_specs=[hbm, hbm, hbm, vmem, vmem],
        out_specs=(vmem, vmem),
        scratch_shapes=[
            pltpu.VMEM((8, 4, 32, COLS), BF),
            pltpu.VMEM((6, 2, 32, WIDE), BF),
            pltpu.VMEM((8, 2, 128, 128), BF),
            pltpu.VMEM((8, 2, 128, 128), BF),
            pltpu.VMEM((8, 8, 128, 128), BF),
            pltpu.VMEM((256, 512), F32),
            pltpu.VMEM((128, 512), F32),
            pltpu.VMEM((8, 4, 16, 128), BF),
            pltpu.VMEM((32, 16, 128), BF),
            pltpu.VMEM((3, 8, 8, 128), F32),
            dma((3,)), dma, dma((4,)), dma, dma((2, 5, 4)), dma((2,)), dma((2,)), dma, dma((8, 2)),
            dma, dma((8, 8)), dma, dma, dma, dma, dma((3,)), dma((3,)),
        ],
        compiler_params=pltpu.CompilerParams(has_side_effects=True, vmem_limit_bytes=48 * 1024 * 1024),
        name="project_and_grow",
    )(chunk, stored_block, stored_site, current_block, weight)


def solution(mesh):
    torus = Mesh(mesh.devices.reshape(2, 4, 8, 4, 2), STATE + BOND)
    in_specs = (
        P(STATE, BOND, None),
        P(STATE, None, BOND, None),
        P(STATE, None, BOND, None),
        P(BOND, None, STATE),
        P(None, BOND, STATE),
        P(),
    )
    out_specs = (P(None, BOND, STATE), P(STATE, BOND, None))
    return jax.shard_map(shards, mesh=torus, in_specs=in_specs, out_specs=out_specs, check_vma=False)
```

```python
import jax
import jax.numpy as jnp
from jax import lax
from jax.experimental import pallas as pl
from jax.experimental.pallas import tpu as pltpu
from jax.sharding import Mesh
from jax.sharding import PartitionSpec as P

BF = jnp.bfloat16
F32 = jnp.float32
STATE = ("yl", "x")
BOND = ("z", "yh", "c")
TURN = (0, 1, 3, 2)
WIDE = 2048
SITE = 512

COMMON = [
    (0, 0), (1, 0), (0, 1), (0, 2), (2, 0), (0, 3),
    (1, 1), (1, 2), (1, 3), (2, 1), (2, 2), (2, 3),
]
UP_ORDER = COMMON + [(3, 0), (3, 1), (3, 2), (3, 3)]
DOWN_ORDER = COMMON + [(3, 2), (3, 3), (3, 0), (3, 1)]
HOPS = {1: 1, 4: 2, 6: 3, 8: 4}
RELAYS = {3: (0,), 6: (1, 2), 8: (3, 4), 10: (5, 6), 11: (7,)}


def slot_up(s):
    return 0 if s == 0 else (7 if s == 4 else 2 * s - 1)


def slot_down(s):
    return 0 if s == 0 else (7 if s == 4 else 2 * s)


def remote(src, dst, send, recv, device):
    return pltpu.make_async_remote_copy(
        src_ref=src, dst_ref=dst, send_sem=send, recv_sem=recv,
        device_id=device, device_id_type=pl.DeviceIdType.MESH,
    )


def lanes_to_halves(low, high):
    lane = lax.broadcasted_iota(jnp.int32, low.shape, 1) // 32
    first = jnp.where(lane == 0, low, jnp.where(lane == 1, pltpu.roll(low, 96, 1),
                      jnp.where(lane == 2, pltpu.roll(high, 64, 1), pltpu.roll(high, 32, 1))))
    second = jnp.where(lane == 0, pltpu.roll(low, 96, 1), jnp.where(lane == 1, pltpu.roll(low, 64, 1),
                       jnp.where(lane == 2, pltpu.roll(high, 32, 1), high)))
    return first, second


def halves_to_lanes(first, second):
    lane = lax.broadcasted_iota(jnp.int32, first.shape, 1) // 32
    low = jnp.where(lane == 0, first, jnp.where(lane == 1, pltpu.roll(second, 32, 1),
                    jnp.where(lane == 2, pltpu.roll(first, 32, 1), pltpu.roll(second, 64, 1))))
    high = jnp.where(lane == 0, pltpu.roll(first, 64, 1), jnp.where(lane == 1, pltpu.roll(second, 96, 1),
                     jnp.where(lane == 2, pltpu.roll(first, 96, 1), second)))
    return low, high


def kernel(env_ref, block_ref, site_ref, edge_ref, current_ref, weight_ref, pen_ref, next_ref,
           rows, stored, edges, now, proj_out, proj_in, moved, grown, grown_in, tiles_out, tiles_in, dots,
           local_sem, y_send, y_recv, z_send, z_recv, s_send, s_recv, p_send, p_recv,
           m_send, m_recv, g_send, g_recv, o_send, o_recv, r_send, r_recv, e_send, ez_recv, ey_recv):
    yl, x, z, yh, c = (lax.axis_index(n) for n in ("yl", "x", "z", "yh", "c"))
    state = yl * 4 + x
    up = {"z": lax.rem(z + 1, 8)}
    down = {"z": lax.rem(z + 7, 8)}
    sibling = {"c": 1 - c}
    partner = {"yl": 1 - yl}
    ahead = {"yh": lax.rem(yh + 1, 4)}
    behind = {"yh": lax.rem(yh + 3, 4)}

    def source(q):
        return lax.rem(yh + TURN[q], 4)

    own = [
        pltpu.make_async_copy(env_ref.at[0], rows.at[0, yh], local_sem.at[0]),
        pltpu.make_async_copy(edge_ref, edges.at[0, yh], local_sem.at[1]),
        pltpu.make_async_copy(block_ref.at[0], stored.at[pl.ds(0, 4), c], local_sem.at[2]),
        pltpu.make_async_copy(site_ref.at[0], stored.at[pl.ds(4, 2), c], local_sem.at[3]),
        pltpu.make_async_copy(current_ref, now, local_sem.at[4]),
    ]
    for copy in own:
        copy.start()

    barrier = pltpu.get_barrier_semaphore()
    near = [up, down] + [{"yh": lax.rem(yh + o, 4)} for o in (1, 2, 3)]
    for o in range(16):
        if o:
            there = lax.rem(state * 2 + c + o, 16)
            near.append({"yl": there // 8, "x": lax.rem(there // 2, 4), "c": lax.rem(there, 2)})
    for device in near:
        pl.semaphore_signal(barrier, inc=1, device_id=device, device_id_type=pl.DeviceIdType.MESH)
    pl.semaphore_wait(barrier, len(near))

    swap = [
        remote(block_ref.at[0], stored.at[pl.ds(0, 4), c], s_send.at[0], s_recv.at[0], sibling),
        remote(site_ref.at[0], stored.at[pl.ds(4, 2), c], s_send.at[1], s_recv.at[1], sibling),
    ]

    def pass_up(s, q):
        block = source(q)
        return remote(rows.at[slot_up(s), block], rows.at[slot_up(s + 1), block],
                      z_send, z_recv.at[0, s + 1, q], up)

    def pass_down(s, q):
        block = source(q)
        return remote(rows.at[slot_down(s), block], rows.at[slot_down(s + 1), block],
                      z_send, z_recv.at[1, s + 1, q], down)

    def give(q):
        return remote(rows.at[0, yh], rows.at[0, yh], y_send, y_recv.at[q],
                      {"yh": lax.rem(yh + 4 - TURN[q], 4)})

    def edge_up(s):
        cut = pl.ds(0, 256 if s == 3 else SITE)
        return remote(edges.at[slot_up(s), yh, :, cut], edges.at[slot_up(s + 1), yh, :, cut],
                      e_send, ez_recv.at[0, s + 1], up)

    def edge_down(s):
        cut = pl.ds(256 if s == 3 else 0, 256 if s == 3 else SITE)
        return remote(edges.at[slot_down(s), yh, :, cut], edges.at[slot_down(s + 1), yh, :, cut],
                      e_send, ez_recv.at[1, s + 1], down)

    def edge_side(t, forward, place, lane):
        here = edges.at[t, place]
        return remote(here, here, e_send, ey_recv.at[t, lane], ahead if forward else behind)

    def edge_spread(t):
        edge_side(t, True, yh, 0).start()
        edge_side(t, False, yh, 1).start()

    def edge_relay(t):
        edge_side(t, True, yh, 0).wait_recv()
        edge_side(t, False, yh, 1).wait_recv()
        if t % 2:
            edge_side(t, False, lax.rem(yh + 1, 4), 2).start()
        else:
            edge_side(t, True, lax.rem(yh + 3, 4), 2).start()

    def edge_hop(s):
        edge_up(s - 1).wait_recv()
        edge_down(s - 1).wait_recv()
        if s < 4:
            edge_up(s).start()
            edge_down(s).start()
            edge_spread(slot_up(s))
            edge_spread(slot_down(s))
        else:
            edge_spread(7)

    own[0].wait()
    pass_up(0, 0).start()
    pass_down(0, 0).start()
    for q in (1, 2, 3):
        give(q).start()
    own[1].wait()
    edge_up(0).start()
    edge_down(0).start()
    for copy in swap:
        copy.start()
    edge_spread(0)

    own[4].wait()
    low, high = (now[:, :, 128 * h:128 * (h + 1)].astype(F32).reshape(128, 128) for h in (0, 1))
    current = lanes_to_halves(low, high)
    own[2].wait()
    own[3].wait()
    for copy in swap:
        copy.wait_recv()
    grown[...] = jnp.zeros_like(grown)

    def row_of(t):
        if t == 7:
            return lax.rem(z + 4, 8)
        d = (t + 1) // 2
        return lax.rem(z + (8 - d if t % 2 else d), 8)

    def to_state(t, same):
        r = row_of(t)
        core = c if same else 1 - c
        return remote(proj_out.at[t, core], proj_in.at[state, c], p_send, p_recv.at[state, c],
                      {"yl": r // 4, "x": lax.rem(r, 4), "c": core})

    def moved_copy(t, other, device, sem):
        k = (1 - yl if other else yl) * 4 + x
        return remote(moved.at[t, k], moved.at[t, k], m_send, m_recv.at[t, sem], device)

    def along_x(t, other):
        return [moved_copy(t, other, {"x": lax.rem(x + o, 4)}, (4 if other else 0) + o) for o in (1, 2, 3)]

    def send_moved(t):
        moved_copy(t, False, partner, 4).start()
        for copy in along_x(t, False):
            copy.start()
        if t == 7:
            for o in (1, 2, 3):
                moved_copy(t, False, {"yl": 1 - yl, "x": lax.rem(x + o, 4)}, 4 + o).start()

    def send_proj(t):
        home = row_of(t) == state

        @pl.when(home)
        def _():
            proj_in[state, c] = proj_out[t, c]

        @pl.when(jnp.logical_not(home))
        def _():
            to_state(t, True).start()

        to_state(t, False).start()

    def product(t, start, stop):
        left = stored[start:stop].reshape(64 * (stop - start), WIDE)
        right = rows[t].reshape(128, WIDE)
        return lax.dot_general(left, right, (((1,), (1,)), ((), ())), preferred_element_type=F32).astype(BF)

    def keep_proj(t, value):
        blocks = value.reshape(4, 2, 32, 128)
        for j in (0, 1):
            proj_out[t, j] = blocks[:, j].reshape(128, 128)

    def multiply(t):
        if t == 7:
            moved[t, state] = product(t, 4, 6)
            send_moved(t)
            keep_proj(t, product(t, 0, 4))
        else:
            both = product(t, 0, 6)
            keep_proj(t, both[0:256])
            moved[t, state] = both[256:384]
            send_moved(t)
        send_proj(t)

    def relay(t):
        moved_copy(t, False, partner, 4).wait_recv()
        for copy in along_x(t, True):
            copy.start()

    def grow(t):
        edge_side(t, t % 2 == 0, yh, 2).wait_recv()
        if t == 7:
            moved_copy(t, False, partner, 4).wait_recv()
        for other in (False, True):
            for copy in along_x(t, other):
                copy.wait_recv()
        for s in (0, 1):
            site = edges[t, :, :, 256 * s:256 * (s + 1)].reshape(128, 256)
            right = moved[t, :, 64 * s:64 * (s + 1), :].reshape(512, 128)
            grown[...] += lax.dot_general(site, right, (((0,), (1,)), ((), ())), preferred_element_type=F32)

    done = []

    def step(t):
        multiply(t)
        done.append(t)
        if len(done) >= 2:
            relay(done[-2])
        if len(done) >= 4:
            grow(done[-4])

    for place in range(16):
        for order, passing, lane, last in ((UP_ORDER, pass_up, 0, (0, 1)), (DOWN_ORDER, pass_down, 1, (2, 3))):
            s, q = order[place]
            if s == 0:
                if lane == 0 and q > 0:
                    give(q).wait_recv()
            else:
                passing(s - 1, q).wait_recv()
            if (s, q) != (0, 0) and (s < 3 or q in last):
                passing(s, q).start()
        if place in HOPS:
            edge_hop(HOPS[place])
        for t in RELAYS.get(place, ()):
            edge_relay(t)
        s, q = UP_ORDER[place]
        if q == 3:
            if s == 0:
                step(0)
            else:
                step(slot_up(s))
                step(slot_down(s))
    relay(6)
    for q in (0, 1):
        pass_up(3, q).wait_recv()
    for q in (2, 3):
        pass_down(3, q).wait_recv()
    multiply(7)
    for t in done[-3:]:
        grow(t)

    for k in range(8):
        for i in (0, 1):
            @pl.when(jnp.logical_or(k != state, i != c))
            def _():
                pltpu.make_async_copy(proj_in.at[k, i], proj_in.at[k, i], p_recv.at[k, i]).wait()
    partial = [
        sum(jnp.sum((proj_in[k, i].astype(F32) * current[i]).reshape(16, 8, 128), axis=0) for i in (0, 1))
        for k in range(8)
    ]
    partial = jnp.concatenate([jnp.sum(p, axis=0, keepdims=True) for p in partial], axis=0)

    places = (x * 2 + c, z, yl * 4 + yh)

    def peer(stage, o):
        there = lax.rem(places[stage] + o, 8)
        if stage == 0:
            return {"x": there // 2, "c": lax.rem(there, 2)}
        if stage == 1:
            return {"z": there}
        return {"yl": there // 4, "yh": lax.rem(there, 4)}

    def exchange(stage, value):
        dots[stage, places[stage]] = value
        for o in range(1, 8):
            here = dots.at[stage, places[stage]]
            remote(here, here, r_send.at[stage], r_recv.at[stage], peer(stage, o)).start()

    def collected(stage):
        seven = dots.at[stage, pl.ds(0, 7)]
        pltpu.make_async_copy(seven, seven, r_recv.at[stage]).wait()
        return jnp.sum(dots[stage], axis=0)

    exchange(0, partial)
    grow(7)
    give_half = remote(grown.at[pl.ds(128 * (1 - c), 128)], grown_in, g_send, g_recv, sibling)
    give_half.start()
    exchange(1, collected(0))
    give_half.wait_recv()

    lane = lax.broadcasted_iota(jnp.int32, (16, 128), 1)
    half = grown.at[pl.ds(pl.multiple_of(128 * c, 128), 128)]
    for d in range(4):
        for pair in range(4):
            cut = pl.ds(128 * pair, 128)
            first = half[pl.ds(32 * d, 16), cut] + grown_in[pl.ds(32 * d, 16), cut]
            second = half[pl.ds(32 * d + 16, 16), cut] + grown_in[pl.ds(32 * d + 16, 16), cut]
            tiles_out[2 * pair, d] = jnp.where(lane < 64, first, pltpu.roll(second, 64, 1)).astype(BF)
            tiles_out[2 * pair + 1, d] = jnp.where(lane < 64, pltpu.roll(first, 64, 1), second).astype(BF)

    place = z * 4 + yh
    for k in range(8):
        for d in range(4):
            to = 2 * c + d // 2
            here = jnp.logical_and(jnp.logical_and(k == state, z == state), jnp.logical_and(to == yh, d % 2 == c))

            @pl.when(here)
            def _():
                pltpu.make_async_copy(tiles_out.at[k, d], tiles_in.at[place], o_recv).start()

            @pl.when(jnp.logical_not(here))
            def _():
                remote(tiles_out.at[k, d], tiles_in.at[place], o_send, o_recv,
                       {"yl": k // 4, "x": k % 4, "z": state, "yh": to, "c": d % 2}).start()

    exchange(2, collected(1))
    total = jnp.sum(collected(2), axis=1, keepdims=True) * (1.0 / 4096.0)
    factor = [total[k:k + 1] * weight_ref[k] for k in range(8)]
    halves = []
    for i in (0, 1):
        value = current[i]
        for k in range(8):
            value = value + factor[k] * proj_in[k, i].astype(F32)
        halves.append(value)
    low, high = halves_to_lanes(*halves)
    pen_ref[:, :, 0:128] = low.reshape(4, 32, 128)
    pen_ref[:, :, 128:256] = high.reshape(4, 32, 128)

    pltpu.make_async_copy(tiles_in, tiles_in, o_recv).wait()
    for p in range(16):
        even = tiles_in[2 * p].astype(F32)
        odd = tiles_in[2 * p + 1].astype(F32)
        cut = slice(128 * p, 128 * (p + 1))
        next_ref[0, 0:16, cut] = jnp.where(lane < 64, even, pltpu.roll(odd, 64, 1)).astype(BF)
        next_ref[0, 16:32, cut] = jnp.where(lane < 64, pltpu.roll(even, 64, 1), odd).astype(BF)

    def drained(ref, sem):
        pltpu.make_async_copy(ref, ref, sem).wait()

    for copy in swap:
        copy.wait_send()
    drained(rows.at[0, pl.ds(0, 3)], y_send)
    drained(rows.at[pl.ds(0, 7)], z_send)
    drained(edges.at[pl.ds(0, 7)], e_send)
    drained(edges.at[0, pl.ds(0, 3)], e_send)
    drained(proj_in.at[pl.ds(0, 7)], p_send)
    drained(proj_in.at[0, 0], p_send)
    drained(moved.at[pl.ds(0, 7)], m_send)
    give_half.wait_send()
    for stage in range(3):
        drained(dots.at[stage, pl.ds(0, 7)], r_send.at[stage])
    drained(tiles_in.at[pl.ds(0, 31)], o_send)

    @pl.when(jnp.logical_not(jnp.logical_and(z == state, yh // 2 == c)))
    def _():
        drained(tiles_in.at[0], o_send)


def shards(intersect_left, stored_block, stored_site, current_site, current_block, penalty_weight):
    hbm = pl.BlockSpec(memory_space=pl.ANY)
    vmem = pl.BlockSpec(memory_space=pltpu.VMEM)
    dma = pltpu.SemaphoreType.DMA
    return pl.pallas_call(
        kernel,
        out_shape=(
            jax.ShapeDtypeStruct((4, 32, 256), F32),
            jax.ShapeDtypeStruct((1, 32, 2048), BF),
        ),
        in_specs=[hbm, hbm, hbm, hbm, hbm, pl.BlockSpec(memory_space=pltpu.SMEM)],
        out_specs=(vmem, vmem),
        scratch_shapes=[
            pltpu.VMEM((8, 4, 32, WIDE), BF),
            pltpu.VMEM((6, 2, 32, WIDE), BF),
            pltpu.VMEM((8, 4, 32, SITE), BF),
            pltpu.VMEM((4, 32, 256), BF),
            pltpu.VMEM((8, 2, 128, 128), BF),
            pltpu.VMEM((8, 2, 128, 128), BF),
            pltpu.VMEM((8, 8, 128, 128), BF),
            pltpu.VMEM((256, 512), F32),
            pltpu.VMEM((128, 512), F32),
            pltpu.VMEM((8, 4, 16, 128), BF),
            pltpu.VMEM((32, 16, 128), BF),
            pltpu.VMEM((3, 8, 8, 128), F32),
            dma((5,)), dma, dma((4,)), dma, dma((2, 5, 4)), dma((2,)), dma((2,)), dma, dma((8, 2)),
            dma, dma((8, 8)), dma, dma, dma, dma, dma((3,)), dma((3,)), dma, dma((2, 5)), dma((8, 3)),
        ],
        compiler_params=pltpu.CompilerParams(collective_id=0, has_side_effects=True, vmem_limit_bytes=63 * 1024 * 1024),
        name="project_and_grow",
    )(intersect_left, stored_block, stored_site, current_site.reshape(32, SITE), current_block, penalty_weight)


def solution(mesh):
    torus = Mesh(mesh.devices.reshape(2, 4, 8, 4, 2), STATE + BOND)
    in_specs = (
        P(STATE, BOND, None),
        P(STATE, None, BOND, None),
        P(STATE, None, BOND, None),
        P(BOND, None, STATE),
        P(None, BOND, STATE),
        P(),
    )
    out_specs = (P(None, BOND, STATE), P(STATE, BOND, None))
    return jax.shard_map(shards, mesh=torus, in_specs=in_specs, out_specs=out_specs, check_vma=False)
```

```python
import jax
import jax.numpy as jnp
from jax import lax
from jax.experimental import pallas as pl
from jax.experimental.pallas import tpu as pltpu
from jax.sharding import Mesh
from jax.sharding import PartitionSpec as P

BF = jnp.bfloat16
F32 = jnp.float32
STATE = ("yl", "x")
BOND = ("z", "yh", "c")
WIDE = 2048
SITE = 512

ORDER = [
    (0, 0), (1, 0), (2, 0), (0, 1), (3, 0), (1, 1), (0, 3), (2, 1),
    (0, 2), (1, 3), (3, 1), (1, 2), (2, 3), (2, 2), (3, 3), (3, 2),
]
UNITS = [(0, 0), (1, 0), (2, 0), (3, 0), (1, 1), (2, 1), (3, 1), (4, 0)]
HOPS = {1: 1, 2: 2, 4: 3, 6: 4}
SPREADS = {3: (0,), 5: (1,), 6: (2,), 7: (3,), 9: (4,)}
RELAYS = {8: (0,), 10: (1,), 11: (2,), 13: (3,), 15: (4,)}
TASKS = {
    5: [(0, 1)],
    6: [(0, 0)],
    7: [(0, 2)],
    8: [(1, 1)],
    10: [(0, 3), (1, 0)],
    11: [(0, 4), (1, 2), (2, 1)],
    13: [(0, 5), (1, 3), (2, 0)],
    14: [(2, 2), (1, 4)],
    15: [(0, 6), (3, 1)],
    16: [(1, 5), (2, 3)],
    17: [(3, 0), (3, 2)],
    19: [(2, 4)],
}


def remote(src, dst, send, recv, device):
    return pltpu.make_async_remote_copy(
        src_ref=src, dst_ref=dst, send_sem=send, recv_sem=recv,
        device_id=device, device_id_type=pl.DeviceIdType.MESH,
    )


def lanes_to_halves(low, high):
    lane = lax.broadcasted_iota(jnp.int32, low.shape, 1) // 32
    first = jnp.where(lane == 0, low, jnp.where(lane == 1, pltpu.roll(low, 96, 1),
                      jnp.where(lane == 2, pltpu.roll(high, 64, 1), pltpu.roll(high, 32, 1))))
    second = jnp.where(lane == 0, pltpu.roll(low, 96, 1), jnp.where(lane == 1, pltpu.roll(low, 64, 1),
                       jnp.where(lane == 2, pltpu.roll(high, 32, 1), high)))
    return first, second


def halves_to_lanes(first, second):
    lane = lax.broadcasted_iota(jnp.int32, first.shape, 1) // 32
    low = jnp.where(lane == 0, first, jnp.where(lane == 1, pltpu.roll(second, 32, 1),
                    jnp.where(lane == 2, pltpu.roll(first, 32, 1), pltpu.roll(second, 64, 1))))
    high = jnp.where(lane == 0, pltpu.roll(first, 64, 1), jnp.where(lane == 1, pltpu.roll(second, 96, 1),
                     jnp.where(lane == 2, pltpu.roll(first, 96, 1), second)))
    return low, high


def turned(low, high, blocks):
    lane = lax.broadcasted_iota(jnp.int32, low.shape, 1)
    a, b = pltpu.roll(low, 64, 1), pltpu.roll(high, 64, 1)
    odd = lax.rem(blocks, 2) == 1
    first = jnp.where(odd, jnp.where(lane < 64, a, b), low)
    second = jnp.where(odd, jnp.where(lane < 64, b, a), high)
    swap = blocks >= 2
    return jnp.where(swap, second, first), jnp.where(swap, first, second)


def kernel(env_ref, block_ref, site_ref, edge_ref, current_ref, weight_ref, pen_ref, next_ref,
           rows, stored, edges, now, proj_out, proj_in, moved, grown, grown_in,
           tiles_out, tiles_in, dots, weights, pen_out, next_out,
           local_sem, y_send, y_recv, d_send, d_recv, z_send, z_recv, s_send, s_recv, p_send, p_recv,
           m_send, m_recv, g_send, g_recv, o_send, o_recv, r_send, r_recv, e_send, ed_recv, ez_recv, ey_recv):
    yl, x, z, yh, c = (lax.axis_index(n) for n in ("yl", "x", "z", "yh", "c"))
    state = yl * 4 + x
    onward = {"z": lax.rem(z + 7 + 2 * c, 8)}
    sibling = {"c": 1 - c}
    partner = {"yl": 1 - yl}

    own = [
        pltpu.make_async_copy(env_ref.at[0], rows.at[0, 0, c], local_sem.at[0]),
        pltpu.make_async_copy(edge_ref, edges.at[0, 0, c], local_sem.at[1]),
        pltpu.make_async_copy(block_ref.at[0], stored.at[pl.ds(0, 4), c], local_sem.at[2]),
        pltpu.make_async_copy(site_ref.at[0], stored.at[pl.ds(4, 2), c], local_sem.at[3]),
        pltpu.make_async_copy(current_ref, now, local_sem.at[4]),
        pltpu.make_async_copy(weight_ref, weights, local_sem.at[5]),
    ]
    for copy in own:
        copy.start()

    barrier = pltpu.get_barrier_semaphore()
    near = [{"z": lax.rem(z + 1, 8)}, {"z": lax.rem(z + 7, 8)}] + [{"yh": lax.rem(yh + o, 4)} for o in (1, 2, 3)]
    for o in range(1, 16):
        there = lax.rem(state * 2 + c + o, 16)
        near.append({"yl": there // 8, "x": lax.rem(there // 2, 4), "c": lax.rem(there, 2)})
    for device in near:
        pl.semaphore_signal(barrier, inc=1, device_id=device, device_id_type=pl.DeviceIdType.MESH)
    pl.semaphore_wait(barrier, len(near))

    swap = [
        remote(block_ref.at[0], stored.at[pl.ds(0, 4), c], s_send.at[0], s_recv.at[0], sibling),
        remote(site_ref.at[0], stored.at[pl.ds(4, 2), c], s_send.at[1], s_recv.at[1], sibling),
    ]

    def passing(s, q, other):
        core = 1 - c if other else c
        return remote(rows.at[s, q, core], rows.at[s + 1, q, core], z_send, z_recv.at[s + 1, q, other], onward)

    def give(q):
        return remote(rows.at[0, 0, c], rows.at[0, q, c], y_send, y_recv.at[q], {"yh": lax.rem(yh + 4 - q, 4)})

    def give_far(q):
        half = pl.ds(0 if q == 1 else 16, 16)
        return remote(rows.at[0, q, c, half], rows.at[0, 2, c, half], y_send, y_recv.at[0 if q == 1 else 2],
                      {"yh": lax.rem(yh + 4 - q, 4)})

    def across(q):
        here = rows.at[0, q, c]
        return remote(here, here, d_send, d_recv.at[q], sibling)

    def edge_of(s, place):
        return edges.at[s, place] if s in (1, 2, 3) else edges.at[s, place, c]

    edge_across = remote(edges.at[0, 0, c], edges.at[0, 0, c], e_send, ed_recv, sibling)

    def edge_on(s):
        if s == 3:
            return remote(edges.at[3, 0, c], edges.at[4, 0, c], e_send, ez_recv.at[4], onward)
        return remote(edges.at[s, 0], edges.at[s + 1, 0], e_send, ez_recv.at[s + 1], onward)

    def edge_side(s, q):
        return remote(edge_of(s, 0), edge_of(s, q), e_send, ey_recv.at[s, q], {"yh": lax.rem(yh + 4 - q, 4)})

    def edge_far(s):
        q = 1 + 2 * lax.rem(c + s, 2)
        return remote(edge_of(s, q), edge_of(s, 2), e_send, ey_recv.at[s, 2], {"yh": lax.rem(yh + 4 - q, 4)})

    def edge_spread(s):
        edge_side(s, 1).start()
        edge_side(s, 3).start()

    def edge_relay(s):
        edge_side(s, 1).wait_recv()
        edge_side(s, 3).wait_recv()
        edge_far(s).start()

    def edge_hop(s):
        edge_on(s - 1).wait_recv()
        if s < 4:
            edge_on(s).start()

    own[0].wait()
    passing(0, 0, 0).start()
    across(0).start()
    for q in (1, 3):
        give(q).start()
    own[1].wait()
    edge_across.start()
    across(0).wait_recv()
    passing(0, 0, 1).start()
    edge_across.wait_recv()
    edge_on(0).start()

    own[4].wait()
    special = lax.rem(state + 8 - z, 4) == 0
    low, high = (now[:, :, 128 * h:128 * (h + 1)].astype(F32).reshape(128, 128) for h in (0, 1))
    low, high = turned(low, high, yh)
    current = [jnp.where(special, mixed, plain) for mixed, plain in zip(lanes_to_halves(low, high), (low, high))]
    grown[...] = jnp.zeros_like(grown)

    def origin(u):
        s = UNITS[u][0]
        return lax.rem(z + 8 + s - 2 * s * c, 8)

    def to_state(u, other, at_home=False):
        r = origin(u)
        core = 1 - c if other else c
        s, pair = UNITS[u]
        cut = pl.ds(128 * pair, 128) if s in (1, 2, 3) else pl.ds(pl.multiple_of(128 * c, 128), 128)
        there = proj_in.at[state, :, cut]
        if at_home:
            return pltpu.make_async_copy(proj_out.at[u, core], there, p_recv.at[state])
        return remote(proj_out.at[u, core], there, p_send.at[u, other], p_recv.at[state],
                      {"yl": r // 4, "x": lax.rem(r, 4), "c": core})

    def moved_copy(s, other, device, sem):
        block = moved.at[s, (1 - yl if other else yl) * 4 + x]
        return remote(block, block, m_send, m_recv.at[s, sem], device)

    def along_x(s, other, steps=(1, 2, 3)):
        return [near_x(s, other, o) for o in steps]

    def near_x(s, other, o):
        return moved_copy(s, other, {"x": lax.rem(x + o, 4)}, (4 if other else 0) + o)

    def far_along_x(s, other):
        step = 3 if other else 1
        block = moved.at[s, (1 - yl if other else yl) * 4 + lax.rem(x + 4 - step, 4)]
        return remote(block, block, m_send, m_recv.at[s, (4 if other else 0) + 2], {"x": lax.rem(x + step, 4)})

    def send_moved(s):
        moved_copy(s, False, partner, 4).start()
        for copy in along_x(s, False, (1, 2, 3) if s == 7 else (1, 3)):
            copy.start()

    def send_proj(s):
        home = origin(s) == state

        @pl.when(home)
        def _():
            to_state(s, 0, True).start()

        @pl.when(jnp.logical_not(home))
        def _():
            to_state(s, 0).start()

        to_state(s, 1).start()

    def unit_of(ref, u):
        s, pair = UNITS[u]
        return ref.at[s, pl.ds(2 * pair, 2)] if s in (1, 2, 3) else ref.at[s, :, c]

    def product(u, start, stop):
        left = stored[start:stop].reshape(64 * (stop - start), WIDE)
        right = unit_of(rows, u)[...].reshape(128, WIDE)
        return lax.dot_general(left, right, (((1,), (1,)), ((), ())), preferred_element_type=F32).astype(BF)

    def keep_proj(u, value):
        blocks = value.reshape(4, 2, 32, 128)
        for j in (0, 1):
            proj_out[u, j] = blocks[:, j].reshape(128, 128)

    def multiply(u):
        if u == 7:
            moved[u, state] = product(u, 4, 6)
            send_moved(u)
            keep_proj(u, product(u, 0, 4))
            send_proj(u)
        else:
            both = product(u, 0, 6)
            keep_proj(u, both[0:256])
            moved[u, state] = both[256:384]
            send_moved(u)
            send_proj(u)

    def relay(s):
        moved_copy(s, False, partner, 4).wait_recv()
        for copy in along_x(s, True, (1, 2, 3) if s == 7 else (1, 3)):
            copy.start()

    def relay_far(s):
        near_x(s, False, 1).wait_recv()
        far_along_x(s, False).start()
        near_x(s, True, 3).wait_recv()
        far_along_x(s, True).start()

    seen = set()

    def grow(u):
        s = UNITS[u][0]
        if s not in seen:
            seen.add(s)
            edge_far(s).wait_recv()
        for other, steps in ((False, (2, 3)), (True, (1, 2))):
            for copy in along_x(u, other, (1, 2, 3) if u == 7 else steps):
                copy.wait_recv()
        site = unit_of(edges, u)[...].reshape(128, SITE)
        for p in (0, 1):
            right = moved[u, :, 64 * p:64 * (p + 1), :].reshape(512, 128)
            grown[...] += lax.dot_general(site[:, 256 * p:256 * (p + 1)], right, (((0,), (1,)), ((), ())),
                                          preferred_element_type=F32)

    def tasks(place):
        for task, u in TASKS.get(place, ()):
            (multiply, relay, relay_far, grow)[task](u)

    for place, (s, q) in enumerate(ORDER):
        if (s, q) == (0, 1):
            for near_q in (1, 3):
                give(near_q).wait_recv()
                give_far(near_q).start()
                across(near_q).start()
        if (s, q) == (0, 3):
            for near_q in (1, 3):
                give_far(near_q).wait_recv()
            across(2).start()
        if s == 0 and q:
            passing(0, q, 0).start()
            across(q).wait_recv()
            passing(0, q, 1).start()
        if s:
            passing(s - 1, q, 0).wait_recv()
            passing(s, q, 0).start()
            passing(s - 1, q, 1).wait_recv()
            if s < 3:
                passing(s, q, 1).start()
        if place == 2:
            for copy in swap:
                copy.start()
        if place == 5:
            own[2].wait()
            own[3].wait()
            for copy in swap:
                copy.wait_recv()
        tasks(place)
        if place in HOPS:
            edge_hop(HOPS[place])
        for t in SPREADS.get(place, ()):
            edge_spread(t)
        for t in RELAYS.get(place, ()):
            edge_relay(t)
    for q in (0, 1, 3, 2):
        passing(3, q, 0).wait_recv()
        tasks(16 + q)
    multiply(7)
    relay(6)
    relay_far(5)
    relay(7)
    relay_far(6)
    for u in (3, 4, 5):
        grow(u)

    for k in range(8):
        pltpu.make_async_copy(proj_in.at[k], proj_in.at[k], p_recv.at[k]).wait()

    def projected(k, i):
        return proj_in[k, :, 128 * i:128 * (i + 1)].astype(F32)

    partial = [
        sum(jnp.sum((projected(k, i) * current[i]).reshape(16, 8, 128), axis=0) for i in (0, 1))
        for k in range(8)
    ]
    across_lanes = lax.broadcasted_iota(jnp.int32, (1, 128), 1)
    partial = sum(
        jnp.where(across_lanes == k, jnp.sum(jnp.sum(p, axis=0, keepdims=True), axis=1, keepdims=True), 0.0)
        for k, p in enumerate(partial)
    )

    places = (state * 2 + c, z * 4 + yh)
    sizes = (16, 32)

    def peer(stage, o):
        there = lax.rem(places[stage] + o, sizes[stage])
        if stage == 0:
            return {"yl": there // 8, "x": lax.rem(there // 2, 4), "c": lax.rem(there, 2)}
        return {"z": there // 4, "yh": lax.rem(there, 4)}

    def exchange(stage, value):
        dots[stage, places[stage]] = value
        for o in range(1, sizes[stage]):
            here = dots.at[stage, places[stage]]
            remote(here, here, r_send.at[stage], r_recv.at[stage], peer(stage, o)).start()

    def collected(stage):
        others = dots.at[stage, pl.ds(0, sizes[stage] - 1)]
        pltpu.make_async_copy(others, others, r_recv.at[stage]).wait()
        return jnp.sum(dots[stage, 0:sizes[stage]], axis=0)

    exchange(0, partial)
    grow(6)
    grow(7)
    give_half = remote(grown.at[pl.ds(128 * (1 - c), 128)], grown_in, g_send, g_recv, sibling)
    give_half.start()
    give_half.wait_recv()

    lane = lax.broadcasted_iota(jnp.int32, (16, 128), 1)
    half = grown.at[pl.ds(pl.multiple_of(128 * c, 128), 128)]
    for d in range(4):
        for pair in range(4):
            cut = pl.ds(128 * pair, 128)
            first = half[pl.ds(32 * d, 16), cut] + grown_in[pl.ds(32 * d, 16), cut]
            second = half[pl.ds(32 * d + 16, 16), cut] + grown_in[pl.ds(32 * d + 16, 16), cut]
            tiles_out[2 * pair, d] = jnp.where(lane < 64, first, pltpu.roll(second, 64, 1)).astype(BF)
            tiles_out[2 * pair + 1, d] = jnp.where(lane < 64, pltpu.roll(first, 64, 1), second).astype(BF)

    place = z * 4 + yh
    for k in range(8):
        for d in range(4):
            to = 2 * c + d // 2
            here = jnp.logical_and(jnp.logical_and(k == state, z == state), jnp.logical_and(to == yh, d % 2 == c))

            @pl.when(here)
            def _():
                pltpu.make_async_copy(tiles_out.at[k, d], tiles_in.at[place], o_recv).start()

            @pl.when(jnp.logical_not(here))
            def _():
                remote(tiles_out.at[k, d], tiles_in.at[place], o_send, o_recv,
                       {"yl": k // 4, "x": k % 4, "z": state, "yh": to, "c": d % 2}).start()

    exchange(1, collected(0))
    own[5].wait()
    total = collected(1) * (1.0 / 4096.0)
    factor = [total[:, k:k + 1] * weights[k] for k in range(8)]
    halves = []
    for i in (0, 1):
        value = current[i]
        for k in range(8):
            value = value + factor[k] * projected(k, i)
        halves.append(value)
    low, high = (jnp.where(special, mixed, plain) for mixed, plain in zip(halves_to_lanes(*halves), halves))
    low, high = turned(low, high, lax.rem(4 - yh, 4))
    pen_out[:, :, 0:128] = low.reshape(4, 32, 128)
    pen_out[:, :, 128:256] = high.reshape(4, 32, 128)

    pen_copy = pltpu.make_async_copy(pen_out, pen_ref, local_sem.at[1])
    pen_copy.start()

    pltpu.make_async_copy(tiles_in, tiles_in, o_recv).wait()
    for p in range(16):
        even = tiles_in[2 * p].astype(F32)
        odd = tiles_in[2 * p + 1].astype(F32)
        cut = slice(128 * p, 128 * (p + 1))
        next_out[ 0:16, cut] = jnp.where(lane < 64, even, pltpu.roll(odd, 64, 1)).astype(BF)
        next_out[ 16:32, cut] = jnp.where(lane < 64, pltpu.roll(even, 64, 1), odd).astype(BF)

    next_copy = pltpu.make_async_copy(next_out, next_ref.at[0], local_sem.at[0])
    next_copy.start()

    def drained(ref, sem):
        pltpu.make_async_copy(ref, ref, sem).wait()

    for copy in swap:
        copy.wait_send()
    drained(rows.at[0, pl.ds(0, 3), 0], y_send)
    drained(rows.at[0, :, 0], d_send)
    drained(rows.at[pl.ds(0, 3)], z_send)
    drained(rows.at[3, :, 0], z_send)
    drained(edges.at[pl.ds(0, 4)], e_send)
    for t in range(8):
        @pl.when(origin(t) != state)
        def _():
            to_state(t, 0).wait_send()

        to_state(t, 1).wait_send()
    drained(moved.at[pl.ds(0, 7)], m_send)
    give_half.wait_send()
    for stage in range(2):
        drained(dots.at[stage, pl.ds(0, sizes[stage] - 1)], r_send.at[stage])
    drained(tiles_in.at[pl.ds(0, 31)], o_send)

    @pl.when(jnp.logical_not(jnp.logical_and(z == state, yh // 2 == c)))
    def _():
        drained(tiles_in.at[0], o_send)
    next_copy.wait()
    pen_copy.wait()


def shards(intersect_left, stored_block, stored_site, current_site, current_block, penalty_weight):
    hbm = pl.BlockSpec(memory_space=pl.ANY)
    dma = pltpu.SemaphoreType.DMA
    return pl.pallas_call(
        kernel,
        out_shape=(
            jax.ShapeDtypeStruct((4, 32, 256), F32),
            jax.ShapeDtypeStruct((1, 32, 2048), BF),
        ),
        in_specs=[hbm] * 6,
        out_specs=(hbm, hbm),
        scratch_shapes=[
            pltpu.VMEM((5, 4, 2, 32, WIDE), BF),
            pltpu.VMEM((6, 2, 32, WIDE), BF),
            pltpu.VMEM((5, 4, 2, 32, SITE), BF),
            pltpu.VMEM((4, 32, 256), BF),
            pltpu.VMEM((8, 2, 128, 128), BF),
            pltpu.VMEM((8, 128, 256), BF),
            pltpu.VMEM((8, 8, 128, 128), BF),
            pltpu.VMEM((256, 512), F32),
            pltpu.VMEM((128, 512), F32),
            pltpu.VMEM((8, 4, 16, 128), BF),
            pltpu.VMEM((32, 16, 128), BF),
            pltpu.VMEM((2, 32, 1, 128), F32),
            pltpu.SMEM((8,), F32),
            pltpu.VMEM((4, 32, 256), F32),
            pltpu.VMEM((32, 2048), BF),
            dma((6,)), dma, dma((4,)), dma, dma((4,)), dma, dma((5, 4, 2)), dma((2,)), dma((2,)), dma((8, 2)), dma((8,)),
            dma, dma((8, 8)), dma, dma, dma, dma, dma((2,)), dma((2,)), dma, dma, dma((5,)), dma((5, 4)),
        ],
        compiler_params=pltpu.CompilerParams(collective_id=0, has_side_effects=True, vmem_limit_bytes=63 * 1024 * 1024),
        name="project_and_grow",
    )(intersect_left, stored_block, stored_site, current_site.reshape(32, SITE), current_block, penalty_weight)


def solution(mesh):
    torus = Mesh(mesh.devices.reshape(2, 4, 8, 4, 2), STATE + BOND)
    in_specs = (
        P(STATE, BOND, None),
        P(STATE, None, BOND, None),
        P(STATE, None, BOND, None),
        P(BOND, None, STATE),
        P(None, BOND, STATE),
        P(),
    )
    out_specs = (P(None, BOND, STATE), P(STATE, BOND, None))
    return jax.shard_map(shards, mesh=torus, in_specs=in_specs, out_specs=out_specs, check_vma=False)
```

```python
import jax
import jax.numpy as jnp
from jax import lax
from jax.experimental import pallas as pl
from jax.experimental.pallas import tpu as pltpu
from jax.sharding import Mesh
from jax.sharding import PartitionSpec as P

BF = jnp.bfloat16
F32 = jnp.float32
STATE = ("yl", "x")
BOND = ("z", "yh", "c")
WIDE = 2048
SITE = 512

ORDER = [
    (0, 0), (1, 0), (2, 0), (0, 1), (3, 0), (1, 1), (0, 3), (2, 1),
    (0, 2), (1, 3), (3, 1), (1, 2), (2, 3), (2, 2), (3, 3), (3, 2),
]
UNITS = [(0, 0), (1, 0), (2, 0), (3, 0), (1, 1), (2, 1), (3, 1), (4, 0)]
HOPS = {1: 1, 2: 2, 4: 3, 6: 4}
SPREADS = {3: (0,), 5: (1,), 7: (2,), 10: (3,), 12: (4,)}
RELAYS = {9: (0,), 11: (1,), 12: (2,), 14: (3,), 15: (4,)}
TASKS = {
    5: [(0, 1)],
    7: [(0, 2)],
    8: [(0, 0), (1, 1)],
    10: [(0, 3)],
    11: [(0, 4), (1, 0), (1, 2), (2, 1)],
    13: [(0, 5), (1, 3), (2, 0)],
    14: [(2, 2), (1, 4)],
    15: [(0, 6), (3, 1)],
    16: [(1, 5), (2, 3)],
    17: [(3, 0), (3, 2)],
    19: [(2, 4)],
}


def remote(src, dst, send, recv, device):
    return pltpu.make_async_remote_copy(
        src_ref=src, dst_ref=dst, send_sem=send, recv_sem=recv,
        device_id=device, device_id_type=pl.DeviceIdType.MESH,
    )


def turned(low, high, blocks):
    lane = lax.broadcasted_iota(jnp.int32, low.shape, 1)
    a, b = pltpu.roll(low, 64, 1), pltpu.roll(high, 64, 1)
    odd = lax.rem(blocks, 2) == 1
    first = jnp.where(odd, jnp.where(lane < 64, a, b), low)
    second = jnp.where(odd, jnp.where(lane < 64, b, a), high)
    swap = blocks >= 2
    return jnp.where(swap, second, first), jnp.where(swap, first, second)


def kernel(env_ref, block_ref, site_ref, edge_ref, current_ref, weight_ref, pen_ref, next_ref,
           rows, stored, edges, now, proj_out, proj_in, moved, grown, grown_in,
           tiles_out, tiles_in, dots, weights, pen_out, next_out, pairs,
           local_sem, sent, y_recv, d_recv, z_recv, s_recv, p_recv, m_recv, g_recv, o_recv, r_recv,
           ed_recv, ez_recv, ey_recv):
    yl, x, z, yh, c = (lax.axis_index(n) for n in ("yl", "x", "z", "yh", "c"))
    state = yl * 4 + x
    onward = {"z": lax.rem(z + 7 + 2 * c, 8)}
    sibling = {"c": 1 - c}
    partner = {"yl": 1 - yl}

    own = [
        pltpu.make_async_copy(env_ref.at[0], rows.at[0, 0, c], local_sem.at[0]),
        pltpu.make_async_copy(edge_ref, pairs, local_sem.at[1]),
        pltpu.make_async_copy(block_ref.at[0], stored.at[pl.ds(0, 4), c], local_sem.at[2]),
        pltpu.make_async_copy(site_ref.at[0], stored.at[pl.ds(4, 2), c], local_sem.at[3]),
        pltpu.make_async_copy(current_ref, now, local_sem.at[4]),
        pltpu.make_async_copy(weight_ref, weights, local_sem.at[5]),
    ]
    for copy in own:
        copy.start()

    barrier = pltpu.get_barrier_semaphore()
    near = [{"z": lax.rem(z + 1, 8)}, {"z": lax.rem(z + 7, 8)}] + [{"yh": lax.rem(yh + o, 4)} for o in (1, 2, 3)]
    for o in range(1, 16):
        there = lax.rem(state * 2 + c + o, 16)
        near.append({"yl": there // 8, "x": lax.rem(there // 2, 4), "c": lax.rem(there, 2)})
    for device in near:
        pl.semaphore_signal(barrier, inc=1, device_id=device, device_id_type=pl.DeviceIdType.MESH)
    own[1].wait()
    for p in (0, 1):
        edges[0, 0, c, :, 256 * p:256 * (p + 1)] = pairs[:, p, :]
    pl.semaphore_wait(barrier, len(near))

    swap = [
        remote(block_ref.at[0], stored.at[pl.ds(0, 4), c], sent, s_recv, sibling),
        remote(site_ref.at[0], stored.at[pl.ds(4, 2), c], sent, s_recv, sibling),
    ]

    def passing(s, q, other):
        core = 1 - c if other else c
        return remote(rows.at[s, q, core], rows.at[s + 1, q, core], sent, z_recv.at[s, q, other], onward)

    def give(q):
        return remote(rows.at[0, 0, c], rows.at[0, q, c], sent, y_recv.at[q], {"yh": lax.rem(yh + 4 - q, 4)})

    def give_far(q):
        half = pl.ds(0 if q == 1 else 16, 16)
        return remote(rows.at[0, q, c, half], rows.at[0, 2, c, half], sent, y_recv.at[0 if q == 1 else 2],
                      {"yh": lax.rem(yh + 4 - q, 4)})

    def across(q):
        here = rows.at[0, q, c]
        return remote(here, here, sent, d_recv.at[q], sibling)

    def edge_of(s, place):
        return edges.at[s, place]

    edge_across = remote(edges.at[0, 0, c], edges.at[0, 0, c], sent, ed_recv, sibling)

    def edge_on(s):
        return remote(edges.at[s, 0], edges.at[s + 1, 0], sent, ez_recv.at[s], onward)

    def edge_side(s, q):
        return remote(edge_of(s, 0), edge_of(s, q), sent, ey_recv.at[s, 0], {"yh": lax.rem(yh + 4 - q, 4)})

    def edge_far(s):
        q = 1 + 2 * lax.rem(c + s, 2) if s in (1, 2, 3) else 3
        return remote(edge_of(s, q), edge_of(s, 2), sent, ey_recv.at[s, 1], {"yh": lax.rem(yh + 4 - q, 4)})

    def edge_spread(s):
        def side(q, core):
            @pl.when(jnp.logical_or(s in (1, 2, 3), c == core))
            def _():
                edge_side(s, q).start()

        side(1, 1)
        side(3, 0)

    def edge_relay(s):
        if s in (1, 2, 3):
            both = edges.at[s, pl.ds(0, 2)]
            pltpu.make_async_copy(both, both, ey_recv.at[s, 0]).wait()
            edge_far(s).start()
        else:
            @pl.when(c == 0)
            def _():
                edge_side(s, 3).wait_recv()
                edge_far(s).start()

    def edge_last(s):
        if s in (1, 2, 3):
            edge_far(s).wait_recv()
        else:
            @pl.when(c == 1)
            def _():
                edge_side(s, 1).wait_recv()

            @pl.when(c == 0)
            def _():
                edge_far(s).wait_recv()

    def edge_hop(s):
        edge_on(s - 1).wait_recv()
        if s < 4:
            edge_on(s).start()

    own[0].wait()
    passing(0, 0, 0).start()
    across(0).start()
    for q in (1, 3):
        give(q).start()
    edge_across.start()
    across(0).wait_recv()
    passing(0, 0, 1).start()
    edge_across.wait_recv()
    edge_on(0).start()

    own[4].wait()
    low, high = (now[:, :, 128 * h:128 * (h + 1)].astype(F32).reshape(128, 128) for h in (0, 1))
    current = turned(low, high, yh)
    grown[...] = jnp.zeros_like(grown)

    def origin(u):
        s = UNITS[u][0]
        return lax.rem(z + 8 + s - 2 * s * c, 8)

    def to_state(u, other, at_home=False):
        r = origin(u)
        core = 1 - c if other else c
        s, pair = UNITS[u]
        cut = pl.ds(128 * pair, 128) if s in (1, 2, 3) else pl.ds(pl.multiple_of(128 * (1 - c), 128), 128)
        there = proj_in.at[state, :, cut]
        if at_home:
            return pltpu.make_async_copy(proj_out.at[u, core], there, p_recv)
        return remote(proj_out.at[u, core], there, sent, p_recv,
                      {"yl": r // 4, "x": lax.rem(r, 4), "c": core})

    def moved_copy(s, other, device, sem):
        block = moved.at[s, (1 - yl if other else yl) * 4 + x]
        return remote(block, block, sent, m_recv.at[s, sem], device)

    def along_x(s, other, steps=(1, 2, 3)):
        return [near_x(s, other, o) for o in steps]

    def near_x(s, other, o):
        return moved_copy(s, other, {"x": lax.rem(x + o, 4)}, 1 if o == (3 if other else 1) else 2)

    def far_along_x(s, other):
        step = 3 if other else 1
        block = moved.at[s, (1 - yl if other else yl) * 4 + lax.rem(x + 4 - step, 4)]
        return remote(block, block, sent, m_recv.at[s, 2], {"x": lax.rem(x + step, 4)})

    def send_moved(s):
        moved_copy(s, False, partner, 0).start()
        for copy in along_x(s, False, (1, 2, 3) if s == 7 else (1, 3)):
            copy.start()

    def send_proj(s):
        home = origin(s) == state

        @pl.when(home)
        def _():
            to_state(s, 0, True).start()

        @pl.when(jnp.logical_not(home))
        def _():
            to_state(s, 0).start()

        to_state(s, 1).start()

    def unit_of(ref, u):
        s, pair = UNITS[u]
        return ref.at[s, pl.ds(2 * pair if s in (1, 2, 3) else 2 * (1 - c), 2)]

    def product(u, start, stop):
        left = stored[start:stop].reshape(64 * (stop - start), WIDE)
        right = unit_of(rows, u)[...].reshape(128, WIDE)
        return lax.dot_general(left, right, (((1,), (1,)), ((), ())), preferred_element_type=F32).astype(BF)

    def keep_proj(u, value):
        blocks = value.reshape(4, 2, 32, 128)
        for j in (0, 1):
            proj_out[u, j] = blocks[:, j].reshape(128, 128)

    def multiply(u):
        if u == 7:
            moved[u, state] = product(u, 4, 6)
            send_moved(u)
            keep_proj(u, product(u, 0, 4))
            send_proj(u)
        else:
            both = product(u, 0, 6)
            keep_proj(u, both[0:256])
            moved[u, state] = both[256:384]
            send_moved(u)
            send_proj(u)

    def moved_here(s, count, sem):
        blocks = moved.at[s, pl.ds(0, count)]
        pltpu.make_async_copy(blocks, blocks, m_recv.at[s, sem]).wait()

    def relay(s):
        moved_copy(s, False, partner, 0).wait_recv()
        for copy in along_x(s, True, (1, 2, 3) if s == 7 else (1, 3)):
            copy.start()

    def relay_far(s):
        moved_here(s, 2, 1)
        far_along_x(s, False).start()
        far_along_x(s, True).start()

    seen = set()

    def grow(u):
        s = UNITS[u][0]
        if s not in seen:
            seen.add(s)
            edge_last(s)
        if u == 7:
            moved_here(u, 2, 1)
        moved_here(u, 4, 2)
        site = unit_of(edges, u)[...].reshape(128, SITE)
        for p in (0, 1):
            right = moved[u, :, 64 * p:64 * (p + 1), :].reshape(512, 128)
            grown[...] += lax.dot_general(site[:, 256 * p:256 * (p + 1)], right, (((0,), (1,)), ((), ())),
                                          preferred_element_type=F32)

    def tasks(place):
        for task, u in TASKS.get(place, ()):
            (multiply, relay, relay_far, grow)[task](u)

    def last_chunks(core, chunks):
        @pl.when(c == core)
        def _():
            for q in chunks:
                for other in (0, 1):
                    passing(3, q, other).wait_recv()

    def last_row(core):
        @pl.when(c == core)
        def _():
            multiply(7)

    for place, (s, q) in enumerate(ORDER):
        if (s, q) == (0, 1):
            for near_q in (1, 3):
                give(near_q).wait_recv()
                give_far(near_q).start()
                across(near_q).start()
        if (s, q) == (0, 3):
            for near_q in (1, 3):
                give_far(near_q).wait_recv()
            across(2).start()
        if s == 0 and q:
            passing(0, q, 0).start()
            across(q).wait_recv()
            passing(0, q, 1).start()
        if s:
            for other in (0, 1):
                passing(s - 1, q, other).wait_recv()

                @pl.when(jnp.logical_or(s < 3, c == (1 if q < 2 else 0)))
                def _():
                    passing(s, q, other).start()
        if place == 2:
            for copy in swap:
                copy.start()
        if place == 5:
            own[2].wait()
            own[3].wait()
            pltpu.make_async_copy(stored.at[:, c], stored.at[:, c], s_recv).wait()
        if place == 13:
            last_chunks(1, (0, 1))
            last_row(1)
        tasks(place)
        if place == 15:
            @pl.when(c == 1)
            def _():
                relay(7)
        if place in HOPS:
            edge_hop(HOPS[place])
        for t in SPREADS.get(place, ()):
            edge_spread(t)
        for t in RELAYS.get(place, ()):
            edge_relay(t)
    tasks(16)
    last_chunks(0, (3,))
    relay(6)
    tasks(17)
    last_chunks(0, (2,))
    last_row(0)
    relay_far(5)
    tasks(19)

    @pl.when(c == 0)
    def _():
        relay(7)

    relay_far(6)
    for u in (3, 4, 5):
        grow(u)

    pltpu.make_async_copy(proj_in, proj_in, p_recv).wait()

    def projected(k, i):
        return proj_in[k, :, 128 * i:128 * (i + 1)].astype(F32)

    partial = [
        sum(jnp.sum((projected(k, i) * current[i]).reshape(16, 8, 128), axis=0) for i in (0, 1))
        for k in range(8)
    ]
    across_lanes = lax.broadcasted_iota(jnp.int32, (1, 128), 1)
    partial = sum(
        jnp.where(across_lanes == k, jnp.sum(jnp.sum(p, axis=0, keepdims=True), axis=1, keepdims=True), 0.0)
        for k, p in enumerate(partial)
    )

    places = (state * 2 + c, z * 4 + yh)
    sizes = (16, 32)

    def peer(stage, o):
        there = lax.rem(places[stage] + o, sizes[stage])
        if stage == 0:
            return {"yl": there // 8, "x": lax.rem(there // 2, 4), "c": lax.rem(there, 2)}
        return {"z": there // 4, "yh": lax.rem(there, 4)}

    def exchange(stage, value):
        dots[stage, places[stage]] = value
        for o in range(1, sizes[stage]):
            here = dots.at[stage, places[stage]]
            remote(here, here, sent, r_recv.at[stage], peer(stage, o)).start()

    def collected(stage):
        others = dots.at[stage, pl.ds(0, sizes[stage] - 1)]
        pltpu.make_async_copy(others, others, r_recv.at[stage]).wait()
        return jnp.sum(dots[stage, 0:sizes[stage]], axis=0)

    exchange(0, partial)
    grow(6)
    grow(7)
    give_half = remote(grown.at[pl.ds(128 * (1 - c), 128)], grown_in, sent, g_recv, sibling)
    give_half.start()
    give_half.wait_recv()

    lane = lax.broadcasted_iota(jnp.int32, (16, 128), 1)
    half = grown.at[pl.ds(pl.multiple_of(128 * c, 128), 128)]
    for d in range(4):
        for pair in range(4):
            cut = pl.ds(128 * pair, 128)
            first = half[pl.ds(32 * d, 16), cut] + grown_in[pl.ds(32 * d, 16), cut]
            second = half[pl.ds(32 * d + 16, 16), cut] + grown_in[pl.ds(32 * d + 16, 16), cut]
            tiles_out[2 * pair, d] = jnp.where(lane < 64, first, pltpu.roll(second, 64, 1)).astype(BF)
            tiles_out[2 * pair + 1, d] = jnp.where(lane < 64, pltpu.roll(first, 64, 1), second).astype(BF)

    place = z * 4 + yh
    for k in range(8):
        for d in range(4):
            to = 2 * c + d // 2
            here = jnp.logical_and(jnp.logical_and(k == state, z == state), jnp.logical_and(to == yh, d % 2 == c))

            @pl.when(here)
            def _():
                pltpu.make_async_copy(tiles_out.at[k, d], tiles_in.at[place], o_recv).start()

            @pl.when(jnp.logical_not(here))
            def _():
                remote(tiles_out.at[k, d], tiles_in.at[place], sent, o_recv,
                       {"yl": k // 4, "x": k % 4, "z": state, "yh": to, "c": d % 2}).start()

    exchange(1, collected(0))
    own[5].wait()
    total = collected(1) * (1.0 / 4096.0)
    factor = [total[:, k:k + 1] * weights[k] for k in range(8)]
    halves = []
    for i in (0, 1):
        value = current[i]
        for k in range(8):
            value = value + factor[k] * projected(k, i)
        halves.append(value)
    low, high = turned(*halves, lax.rem(4 - yh, 4))
    pen_out[:, :, 0:128] = low.reshape(4, 32, 128)
    pen_out[:, :, 128:256] = high.reshape(4, 32, 128)

    pen_copy = pltpu.make_async_copy(pen_out, pen_ref, local_sem.at[1])
    pen_copy.start()

    pltpu.make_async_copy(tiles_in, tiles_in, o_recv).wait()
    for p in range(16):
        even = tiles_in[2 * p].astype(F32)
        odd = tiles_in[2 * p + 1].astype(F32)
        cut = slice(128 * p, 128 * (p + 1))
        next_out[ 0:16, cut] = jnp.where(lane < 64, even, pltpu.roll(odd, 64, 1)).astype(BF)
        next_out[ 16:32, cut] = jnp.where(lane < 64, pltpu.roll(even, 64, 1), odd).astype(BF)

    next_copy = pltpu.make_async_copy(next_out, next_ref.at[0], local_sem.at[0])
    next_copy.start()

    def drained(ref, sem):
        pltpu.make_async_copy(ref, ref, sem).wait()

    drained(stored.at[:, c], sent)
    drained(rows.at[0, pl.ds(0, 3), 0], sent)
    drained(rows.at[0, :, 0], sent)
    drained(rows.at[pl.ds(0, 3)], sent)
    drained(rows.at[3, :, 0], sent)
    drained(edges.at[pl.ds(0, 3)], sent)
    drained(edges.at[3, pl.ds(0, 3)], sent)
    drained(edges.at[3, 3, 0], sent)

    @pl.when(c == 0)
    def _():
        drained(edges.at[0, pl.ds(0, 2)], sent)

    for t in range(8):
        @pl.when(origin(t) != state)
        def _():
            drained(proj_out.at[0, 0], sent)

    drained(proj_out.at[pl.ds(0, 4)], sent)
    drained(moved.at[pl.ds(0, 7)], sent)
    drained(grown_in, sent)
    for stage in range(2):
        drained(dots.at[stage, pl.ds(0, sizes[stage] - 1)], sent)
    drained(tiles_in.at[pl.ds(0, 31)], sent)

    @pl.when(jnp.logical_not(jnp.logical_and(z == state, yh // 2 == c)))
    def _():
        drained(tiles_in.at[0], sent)
    next_copy.wait()
    pen_copy.wait()


def shards(intersect_left, stored_block, stored_site, current_site, current_block, penalty_weight):
    hbm = pl.BlockSpec(memory_space=pl.ANY)
    dma = pltpu.SemaphoreType.DMA
    return pl.pallas_call(
        kernel,
        out_shape=(
            jax.ShapeDtypeStruct((4, 32, 256), F32),
            jax.ShapeDtypeStruct((1, 32, 2048), BF),
        ),
        in_specs=[hbm] * 6,
        out_specs=(hbm, hbm),
        scratch_shapes=[
            pltpu.VMEM((5, 4, 2, 32, WIDE), BF),
            pltpu.VMEM((6, 2, 32, WIDE), BF),
            pltpu.VMEM((5, 4, 2, 32, SITE), BF),
            pltpu.VMEM((4, 32, 256), BF),
            pltpu.VMEM((8, 2, 128, 128), BF),
            pltpu.VMEM((8, 128, 256), BF),
            pltpu.VMEM((8, 8, 128, 128), BF),
            pltpu.VMEM((256, 512), F32),
            pltpu.VMEM((128, 512), F32),
            pltpu.VMEM((8, 4, 16, 128), BF),
            pltpu.VMEM((32, 16, 128), BF),
            pltpu.VMEM((2, 32, 1, 128), F32),
            pltpu.SMEM((8,), F32),
            pltpu.VMEM((4, 32, 256), F32),
            pltpu.VMEM((32, 2048), BF),
            pltpu.VMEM((32, 2, 256), BF),
            dma((6,)), dma, dma((4,)), dma((4,)), dma((4, 4, 2)), dma, dma, dma((8, 3)), dma, dma, dma((2,)),
            dma, dma((4,)), dma((5, 2)),
        ],
        compiler_params=pltpu.CompilerParams(collective_id=0, has_side_effects=True, vmem_limit_bytes=63 * 1024 * 1024),
        name="project_and_grow",
    )(intersect_left, stored_block, stored_site, current_site, current_block, penalty_weight)


def solution(mesh):
    torus = Mesh(mesh.devices.reshape(2, 4, 8, 4, 2), STATE + BOND)
    in_specs = (
        P(STATE, BOND, None),
        P(STATE, None, BOND, None),
        P(STATE, None, BOND, None),
        P(BOND, None, STATE),
        P(None, BOND, STATE),
        P(),
    )
    out_specs = (P(None, BOND, STATE), P(STATE, BOND, None))
    return jax.shard_map(shards, mesh=torus, in_specs=in_specs, out_specs=out_specs, check_vma=False)
```

```python
import jax
import jax.numpy as jnp
from jax import lax
from jax.experimental import pallas as pl
from jax.experimental.pallas import tpu as pltpu
from jax.sharding import Mesh
from jax.sharding import PartitionSpec as P

BF = jnp.bfloat16
F32 = jnp.float32
STATE = ("yl", "x")
BOND = ("z", "yh", "c")
WIDE = 2048
SITE = 512

ORDER = [
    (0, 0), (1, 0), (2, 0), (0, 1), (3, 0), (1, 1), (0, 3), (2, 1),
    (0, 2), (1, 3), (3, 1), (1, 2), (2, 3), (2, 2), (3, 3), (3, 2),
]
UNITS = [(0, 0), (1, 0), (2, 0), (3, 0), (1, 1), (2, 1), (3, 1), (4, 0)]
HOPS = {1: 1, 2: 2, 4: 3, 6: 4}
SPREADS = {3: (0,), 5: (1,), 7: (2,), 10: (3,), 12: (4,)}
RELAYS = {9: (0,), 11: (1,), 12: (2,), 14: (3,), 15: (4,)}
TASKS = {
    5: [(0, 1)],
    7: [(0, 2)],
    8: [(0, 0), (1, 1)],
    10: [(0, 3)],
    11: [(0, 4), (1, 0), (1, 2), (2, 1)],
    13: [(0, 5), (1, 3), (2, 0)],
    14: [(2, 2), (1, 4)],
    15: [(0, 6), (3, 1)],
    16: [(1, 5), (2, 3)],
    17: [(3, 0), (3, 2)],
    19: [(2, 4)],
}


def remote(src, dst, send, recv, device):
    return pltpu.make_async_remote_copy(
        src_ref=src, dst_ref=dst, send_sem=send, recv_sem=recv,
        device_id=device, device_id_type=pl.DeviceIdType.MESH,
    )


def turned(low, high, blocks):
    lane = lax.broadcasted_iota(jnp.int32, low.shape, 1)
    a, b = pltpu.roll(low, 64, 1), pltpu.roll(high, 64, 1)
    odd = lax.rem(blocks, 2) == 1
    first = jnp.where(odd, jnp.where(lane < 64, a, b), low)
    second = jnp.where(odd, jnp.where(lane < 64, b, a), high)
    swap = blocks >= 2
    return jnp.where(swap, second, first), jnp.where(swap, first, second)


def kernel(env_ref, block_ref, site_ref, edge_ref, current_ref, weight_ref, pen_ref, next_ref,
           rows, stored, edges, now, proj_out, proj_in, moved, grown, grown_in,
           tiles_out, tiles_in, dots, weights, pen_out, next_out, pairs,
           local_sem, sent, y_recv, d_recv, z_recv, s_recv, p_recv, m_recv, g_recv, o_recv, r_recv,
           ed_recv, ez_recv, ey_recv):
    yl, x, z, yh, c = (lax.axis_index(n) for n in ("yl", "x", "z", "yh", "c"))
    state = yl * 4 + x
    onward = {"z": lax.rem(z + 7 + 2 * c, 8)}
    sibling = {"c": 1 - c}
    partner = {"yl": 1 - yl}

    barrier = pltpu.get_barrier_semaphore()
    near = [{"z": lax.rem(z + 1, 8)}, {"z": lax.rem(z + 7, 8)}] + [{"yh": lax.rem(yh + o, 4)} for o in (1, 2, 3)]
    for o in range(1, 16):
        there = lax.rem(state * 2 + c + o, 16)
        near.append({"yl": there // 8, "x": lax.rem(there // 2, 4), "c": lax.rem(there, 2)})
    for device in near:
        pl.semaphore_signal(barrier, inc=1, device_id=device, device_id_type=pl.DeviceIdType.MESH)
    own = [
        pltpu.make_async_copy(env_ref.at[0], rows.at[0, 0, c], local_sem.at[0]),
        pltpu.make_async_copy(edge_ref, pairs, local_sem.at[1]),
        pltpu.make_async_copy(block_ref.at[0], stored.at[pl.ds(0, 4), c], local_sem.at[2]),
        pltpu.make_async_copy(site_ref.at[0], stored.at[pl.ds(4, 2), c], local_sem.at[3]),
        pltpu.make_async_copy(current_ref, now, local_sem.at[4]),
        pltpu.make_async_copy(weight_ref, weights, local_sem.at[5]),
    ]
    for copy in own:
        copy.start()

    own[1].wait()
    for p in (0, 1):
        edges[0, 0, c, :, 256 * p:256 * (p + 1)] = pairs[:, p, :]
    pl.semaphore_wait(barrier, len(near))

    swap = [
        remote(block_ref.at[0], stored.at[pl.ds(0, 4), c], sent, s_recv, sibling),
        remote(site_ref.at[0], stored.at[pl.ds(4, 2), c], sent, s_recv, sibling),
    ]

    def passing(s, q, other):
        core = 1 - c if other else c
        return remote(rows.at[s, q, core], rows.at[s + 1, q, core], sent, z_recv.at[s, q, other], onward)

    def give(q):
        return remote(rows.at[0, 0, c], rows.at[0, q, c], sent, y_recv.at[q], {"yh": lax.rem(yh + 4 - q, 4)})

    def give_far(q):
        half = pl.ds(0 if q == 1 else 16, 16)
        return remote(rows.at[0, q, c, half], rows.at[0, 2, c, half], sent, y_recv.at[0 if q == 1 else 2],
                      {"yh": lax.rem(yh + 4 - q, 4)})

    def across(q):
        here = rows.at[0, q, c]
        return remote(here, here, sent, d_recv.at[q], sibling)

    def edge_of(s, place):
        return edges.at[s, place]

    edge_across = remote(edges.at[0, 0, c], edges.at[0, 0, c], sent, ed_recv, sibling)

    def edge_on(s):
        return remote(edges.at[s, 0], edges.at[s + 1, 0], sent, ez_recv.at[s], onward)

    def edge_side(s, q):
        return remote(edge_of(s, 0), edge_of(s, q), sent, ey_recv.at[s, 0], {"yh": lax.rem(yh + 4 - q, 4)})

    def edge_far(s):
        q = 1 + 2 * lax.rem(c + s, 2) if s in (1, 2, 3) else 3
        return remote(edge_of(s, q), edge_of(s, 2), sent, ey_recv.at[s, 1], {"yh": lax.rem(yh + 4 - q, 4)})

    def edge_spread(s):
        def side(q, core):
            @pl.when(jnp.logical_or(s in (1, 2, 3), c == core))
            def _():
                edge_side(s, q).start()

        side(1, 1)
        side(3, 0)

    def edge_relay(s):
        if s in (1, 2, 3):
            both = edges.at[s, pl.ds(0, 2)]
            pltpu.make_async_copy(both, both, ey_recv.at[s, 0]).wait()
            edge_far(s).start()
        else:
            @pl.when(c == 0)
            def _():
                edge_side(s, 3).wait_recv()
                edge_far(s).start()

    def edge_last(s):
        if s in (1, 2, 3):
            edge_far(s).wait_recv()
        else:
            @pl.when(c == 1)
            def _():
                edge_side(s, 1).wait_recv()

            @pl.when(c == 0)
            def _():
                edge_far(s).wait_recv()

    def edge_hop(s):
        edge_on(s - 1).wait_recv()
        if s < 4:
            edge_on(s).start()

    own[0].wait()
    passing(0, 0, 0).start()
    across(0).start()
    for q in (1, 3):
        give(q).start()
    edge_across.start()
    across(0).wait_recv()
    passing(0, 0, 1).start()
    edge_across.wait_recv()
    edge_on(0).start()

    own[4].wait()
    low, high = (now[:, :, 128 * h:128 * (h + 1)].astype(F32).reshape(128, 128) for h in (0, 1))
    current = turned(low, high, yh)
    grown[...] = jnp.zeros_like(grown)

    def origin(u):
        s = UNITS[u][0]
        return lax.rem(z + 8 + s - 2 * s * c, 8)

    def to_state(u, other, at_home=False):
        r = origin(u)
        core = 1 - c if other else c
        s, pair = UNITS[u]
        cut = pl.ds(128 * pair, 128) if s in (1, 2, 3) else pl.ds(pl.multiple_of(128 * (1 - c), 128), 128)
        there = proj_in.at[state, :, cut]
        if at_home:
            return pltpu.make_async_copy(proj_out.at[u, core], there, p_recv)
        return remote(proj_out.at[u, core], there, sent, p_recv,
                      {"yl": r // 4, "x": lax.rem(r, 4), "c": core})

    def moved_copy(s, other, device, sem):
        block = moved.at[s, (1 - yl if other else yl) * 4 + x]
        return remote(block, block, sent, m_recv.at[s, sem], device)

    def along_x(s, other, steps=(1, 2, 3)):
        return [near_x(s, other, o) for o in steps]

    def near_x(s, other, o):
        return moved_copy(s, other, {"x": lax.rem(x + o, 4)}, 1 if o == (3 if other else 1) else 2)

    def far_along_x(s, other):
        step = 3 if other else 1
        block = moved.at[s, (1 - yl if other else yl) * 4 + lax.rem(x + 4 - step, 4)]
        return remote(block, block, sent, m_recv.at[s, 2], {"x": lax.rem(x + step, 4)})

    def send_moved(s):
        moved_copy(s, False, partner, 0).start()
        for copy in along_x(s, False, (1, 3)):
            copy.start()
        if s == 7:
            @pl.when(c == 0)
            def _():
                near_x(s, False, 2).start()

    def send_proj(s):
        home = origin(s) == state

        @pl.when(home)
        def _():
            to_state(s, 0, True).start()

        @pl.when(jnp.logical_not(home))
        def _():
            to_state(s, 0).start()

        to_state(s, 1).start()

    def unit_of(ref, u):
        s, pair = UNITS[u]
        return ref.at[s, pl.ds(2 * pair if s in (1, 2, 3) else 2 * (1 - c), 2)]

    def product(u, start, stop):
        left = stored[start:stop].reshape(64 * (stop - start), WIDE)
        right = unit_of(rows, u)[...].reshape(128, WIDE)
        return lax.dot_general(left, right, (((1,), (1,)), ((), ())), preferred_element_type=F32).astype(BF)

    def keep_proj(u, value):
        blocks = value.reshape(4, 2, 32, 128)
        for j in (0, 1):
            proj_out[u, j] = blocks[:, j].reshape(128, 128)

    def multiply(u):
        if u == 7:
            moved[u, state] = product(u, 4, 6)
            send_moved(u)
            keep_proj(u, product(u, 0, 4))
            send_proj(u)
        else:
            both = product(u, 0, 6)
            keep_proj(u, both[0:256])
            moved[u, state] = both[256:384]
            send_moved(u)
            send_proj(u)

    def moved_here(s, count, sem):
        blocks = moved.at[s, pl.ds(0, count)]
        pltpu.make_async_copy(blocks, blocks, m_recv.at[s, sem]).wait()

    def relay(s):
        moved_copy(s, False, partner, 0).wait_recv()
        for copy in along_x(s, True, (1, 3)):
            copy.start()
        if s == 7:
            @pl.when(c == 0)
            def _():
                near_x(s, True, 2).start()

    def relay_far(s):
        moved_here(s, 2, 1)
        far_along_x(s, False).start()
        far_along_x(s, True).start()

    seen = set()

    def grow(u):
        s = UNITS[u][0]
        if s not in seen:
            seen.add(s)
            edge_last(s)
        if u == 7:
            @pl.when(c == 0)
            def _():
                moved_here(u, 2, 1)

        moved_here(u, 4, 2)
        site = unit_of(edges, u)[...].reshape(128, SITE)
        for p in (0, 1):
            right = moved[u, :, 64 * p:64 * (p + 1), :].reshape(512, 128)
            grown[...] += lax.dot_general(site[:, 256 * p:256 * (p + 1)], right, (((0,), (1,)), ((), ())),
                                          preferred_element_type=F32)

    def tasks(place):
        for task, u in TASKS.get(place, ()):
            (multiply, relay, relay_far, grow)[task](u)

    def last_chunks(core, chunks):
        @pl.when(c == core)
        def _():
            for q in chunks:
                for other in (0, 1):
                    passing(3, q, other).wait_recv()

    def last_row(core):
        @pl.when(c == core)
        def _():
            multiply(7)

    for place, (s, q) in enumerate(ORDER):
        if (s, q) == (0, 1):
            for near_q in (1, 3):
                give(near_q).wait_recv()
                give_far(near_q).start()
                across(near_q).start()
        if (s, q) == (0, 3):
            for near_q in (1, 3):
                give_far(near_q).wait_recv()
            across(2).start()
        if s == 0 and q:
            passing(0, q, 0).start()
            across(q).wait_recv()
            passing(0, q, 1).start()
        if s:
            for other in (0, 1):
                passing(s - 1, q, other).wait_recv()

                @pl.when(jnp.logical_or(s < 3, c == (1 if q < 2 else 0)))
                def _():
                    passing(s, q, other).start()
        if place == 1:
            for copy in swap:
                copy.start()
        if place == 5:
            own[2].wait()
            own[3].wait()
            pltpu.make_async_copy(stored.at[:, c], stored.at[:, c], s_recv).wait()
        if place == 13:
            last_chunks(1, (0, 1))
            last_row(1)
        tasks(place)
        if place == 15:
            @pl.when(c == 1)
            def _():
                relay(7)
        if place in HOPS:
            edge_hop(HOPS[place])
        for t in SPREADS.get(place, ()):
            edge_spread(t)
        for t in RELAYS.get(place, ()):
            edge_relay(t)
    tasks(16)
    last_chunks(0, (3,))
    relay(6)
    tasks(17)

    @pl.when(c == 1)
    def _():
        relay_far(7)

    last_chunks(0, (2,))
    last_row(0)
    relay_far(5)
    tasks(19)

    @pl.when(c == 0)
    def _():
        relay(7)

    relay_far(6)
    for u in (3, 4, 5):
        grow(u)

    pltpu.make_async_copy(proj_in, proj_in, p_recv).wait()

    def projected(k, i):
        return proj_in[k, :, 128 * i:128 * (i + 1)].astype(F32)

    partial = [
        sum(jnp.sum((projected(k, i) * current[i]).reshape(16, 8, 128), axis=0) for i in (0, 1))
        for k in range(8)
    ]
    across_lanes = lax.broadcasted_iota(jnp.int32, (1, 128), 1)
    partial = sum(
        jnp.where(across_lanes == k, jnp.sum(jnp.sum(p, axis=0, keepdims=True), axis=1, keepdims=True), 0.0)
        for k, p in enumerate(partial)
    )

    places = (state * 2 + c, z * 4 + yh)
    sizes = (16, 32)

    def peer(stage, o):
        there = lax.rem(places[stage] + o, sizes[stage])
        if stage == 0:
            return {"yl": there // 8, "x": lax.rem(there // 2, 4), "c": lax.rem(there, 2)}
        return {"z": there // 4, "yh": lax.rem(there, 4)}

    def exchange(stage, value):
        dots[stage, places[stage]] = value
        for o in range(1, sizes[stage]):
            here = dots.at[stage, places[stage]]
            remote(here, here, sent, r_recv.at[stage], peer(stage, o)).start()

    def collected(stage):
        others = dots.at[stage, pl.ds(0, sizes[stage] - 1)]
        pltpu.make_async_copy(others, others, r_recv.at[stage]).wait()
        return jnp.sum(dots[stage, 0:sizes[stage]], axis=0)

    exchange(0, partial)
    grow(6)
    grow(7)
    give_half = remote(grown.at[pl.ds(128 * (1 - c), 128)], grown_in, sent, g_recv, sibling)
    give_half.start()
    give_half.wait_recv()

    lane = lax.broadcasted_iota(jnp.int32, (16, 128), 1)
    half = grown.at[pl.ds(pl.multiple_of(128 * c, 128), 128)]
    for d in range(4):
        for pair in range(4):
            cut = pl.ds(128 * pair, 128)
            first = half[pl.ds(32 * d, 16), cut] + grown_in[pl.ds(32 * d, 16), cut]
            second = half[pl.ds(32 * d + 16, 16), cut] + grown_in[pl.ds(32 * d + 16, 16), cut]
            tiles_out[2 * pair, d] = jnp.where(lane < 64, first, pltpu.roll(second, 64, 1)).astype(BF)
            tiles_out[2 * pair + 1, d] = jnp.where(lane < 64, pltpu.roll(first, 64, 1), second).astype(BF)

    place = z * 4 + yh
    for k in range(8):
        for d in range(4):
            to = 2 * c + d // 2
            here = jnp.logical_and(jnp.logical_and(k == state, z == state), jnp.logical_and(to == yh, d % 2 == c))

            @pl.when(here)
            def _():
                pltpu.make_async_copy(tiles_out.at[k, d], tiles_in.at[place], o_recv).start()

            @pl.when(jnp.logical_not(here))
            def _():
                remote(tiles_out.at[k, d], tiles_in.at[place], sent, o_recv,
                       {"yl": k // 4, "x": k % 4, "z": state, "yh": to, "c": d % 2}).start()

    exchange(1, collected(0))
    own[5].wait()
    total = collected(1) * (1.0 / 4096.0)
    factor = [total[:, k:k + 1] * weights[k] for k in range(8)]
    halves = []
    for i in (0, 1):
        value = current[i]
        for k in range(8):
            value = value + factor[k] * projected(k, i)
        halves.append(value)
    low, high = turned(*halves, lax.rem(4 - yh, 4))
    pen_out[:, :, 0:128] = low.reshape(4, 32, 128)
    pen_out[:, :, 128:256] = high.reshape(4, 32, 128)

    pen_copy = pltpu.make_async_copy(pen_out, pen_ref, local_sem.at[1])
    pen_copy.start()

    pltpu.make_async_copy(tiles_in, tiles_in, o_recv).wait()
    for p in range(16):
        even = tiles_in[2 * p].astype(F32)
        odd = tiles_in[2 * p + 1].astype(F32)
        cut = slice(128 * p, 128 * (p + 1))
        next_out[ 0:16, cut] = jnp.where(lane < 64, even, pltpu.roll(odd, 64, 1)).astype(BF)
        next_out[ 16:32, cut] = jnp.where(lane < 64, pltpu.roll(even, 64, 1), odd).astype(BF)

    next_copy = pltpu.make_async_copy(next_out, next_ref.at[0], local_sem.at[0])
    next_copy.start()

    def drained(ref, sem):
        pltpu.make_async_copy(ref, ref, sem).wait()

    drained(stored.at[:, c], sent)
    drained(rows.at[0, pl.ds(0, 3), 0], sent)
    drained(rows.at[0, :, 0], sent)
    drained(rows.at[pl.ds(0, 3)], sent)
    drained(rows.at[3, :, 0], sent)
    drained(edges.at[pl.ds(0, 3)], sent)
    drained(edges.at[3, pl.ds(0, 3)], sent)
    drained(edges.at[3, 3, 0], sent)

    @pl.when(c == 0)
    def _():
        drained(edges.at[0, pl.ds(0, 2)], sent)

    for t in range(8):
        @pl.when(origin(t) != state)
        def _():
            drained(proj_out.at[0, 0], sent)

    drained(proj_out.at[pl.ds(0, 4)], sent)
    drained(moved.at[pl.ds(0, 7)], sent)
    drained(grown_in, sent)
    for stage in range(2):
        drained(dots.at[stage, pl.ds(0, sizes[stage] - 1)], sent)
    drained(tiles_in.at[pl.ds(0, 31)], sent)

    @pl.when(jnp.logical_not(jnp.logical_and(z == state, yh // 2 == c)))
    def _():
        drained(tiles_in.at[0], sent)
    next_copy.wait()
    pen_copy.wait()


def shards(intersect_left, stored_block, stored_site, current_site, current_block, penalty_weight):
    hbm = pl.BlockSpec(memory_space=pl.ANY)
    dma = pltpu.SemaphoreType.DMA
    return pl.pallas_call(
        kernel,
        out_shape=(
            jax.ShapeDtypeStruct((4, 32, 256), F32),
            jax.ShapeDtypeStruct((1, 32, 2048), BF),
        ),
        in_specs=[hbm] * 6,
        out_specs=(hbm, hbm),
        scratch_shapes=[
            pltpu.VMEM((5, 4, 2, 32, WIDE), BF),
            pltpu.VMEM((6, 2, 32, WIDE), BF),
            pltpu.VMEM((5, 4, 2, 32, SITE), BF),
            pltpu.VMEM((4, 32, 256), BF),
            pltpu.VMEM((8, 2, 128, 128), BF),
            pltpu.VMEM((8, 128, 256), BF),
            pltpu.VMEM((8, 8, 128, 128), BF),
            pltpu.VMEM((256, 512), F32),
            pltpu.VMEM((128, 512), F32),
            pltpu.VMEM((8, 4, 16, 128), BF),
            pltpu.VMEM((32, 16, 128), BF),
            pltpu.VMEM((2, 32, 1, 128), F32),
            pltpu.SMEM((8,), F32),
            pltpu.VMEM((4, 32, 256), F32),
            pltpu.VMEM((32, 2048), BF),
            pltpu.VMEM((32, 2, 256), BF),
            dma((6,)), dma, dma((4,)), dma((4,)), dma((4, 4, 2)), dma, dma, dma((8, 3)), dma, dma, dma((2,)),
            dma, dma((4,)), dma((5, 2)),
        ],
        compiler_params=pltpu.CompilerParams(collective_id=0, has_side_effects=True, vmem_limit_bytes=63 * 1024 * 1024),
        name="project_and_grow",
    )(intersect_left, stored_block, stored_site, current_site, current_block, penalty_weight)


def solution(mesh):
    torus = Mesh(mesh.devices.reshape(2, 4, 8, 4, 2), STATE + BOND)
    in_specs = (
        P(STATE, BOND, None),
        P(STATE, None, BOND, None),
        P(STATE, None, BOND, None),
        P(BOND, None, STATE),
        P(None, BOND, STATE),
        P(),
    )
    out_specs = (P(None, BOND, STATE), P(STATE, BOND, None))
    return jax.shard_map(shards, mesh=torus, in_specs=in_specs, out_specs=out_specs, check_vma=False)
```

```python
import jax
import jax.numpy as jnp
from jax import lax
from jax.experimental import pallas as pl
from jax.experimental.pallas import tpu as pltpu
from jax.sharding import Mesh
from jax.sharding import PartitionSpec as P

BF = jnp.bfloat16
F32 = jnp.float32
STATE = ("yl", "x")
BOND = ("z", "yh", "c")
WIDE = 2048
SITE = 512

ORDER = [
    (0, 0), (1, 0), (2, 0), (0, 1), (3, 0), (1, 1), (0, 3), (2, 1),
    (0, 2), (1, 3), (3, 1), (1, 2), (2, 3), (2, 2), (3, 3), (3, 2),
]
UNITS = [(0, 0), (1, 0), (2, 0), (3, 0), (1, 1), (2, 1), (3, 1), (4, 0)]
HOPS = {1: 1, 2: 2, 4: 3, 6: 4}
SPREADS = {3: (0,), 5: (1,), 7: (2,), 10: (3,), 12: (4,)}
RELAYS = {9: (0,), 11: (1,), 12: (2,), 14: (3,), 15: (4,)}
TASKS = {
    5: [(0, 1)],
    7: [(0, 2)],
    8: [(1, 1)],
    10: [(0, 3)],
    11: [(0, 4), (1, 2), (2, 1)],
    13: [(0, 5), (1, 3)],
    14: [(2, 2), (1, 4)],
    15: [(0, 6), (3, 1)],
    16: [(1, 5), (2, 3)],
    17: [(3, 0), (3, 2)],
    19: [(2, 4)],
}


def remote(src, dst, send, recv, device):
    return pltpu.make_async_remote_copy(
        src_ref=src, dst_ref=dst, send_sem=send, recv_sem=recv,
        device_id=device, device_id_type=pl.DeviceIdType.MESH,
    )


def turned(low, high, blocks):
    lane = lax.broadcasted_iota(jnp.int32, low.shape, 1)
    a, b = pltpu.roll(low, 64, 1), pltpu.roll(high, 64, 1)
    odd = lax.rem(blocks, 2) == 1
    first = jnp.where(odd, jnp.where(lane < 64, a, b), low)
    second = jnp.where(odd, jnp.where(lane < 64, b, a), high)
    swap = blocks >= 2
    return jnp.where(swap, second, first), jnp.where(swap, first, second)


def kernel(env_ref, block_ref, site_ref, edge_ref, current_ref, weight_ref, pen_ref, next_ref,
           rows, stored, edges, now, proj_out, proj_in, moved, grown, grown_in,
           tiles_out, tiles_in, dots, weights, pen_out, next_out, pairs,
           local_sem, sent, y_recv, d_recv, z_recv, s_recv, p_recv, m_recv, g_recv, o_recv, r_recv,
           ed_recv, ez_recv, ey_recv):
    yl, x, z, yh, c = (lax.axis_index(n) for n in ("yl", "x", "z", "yh", "c"))
    state = yl * 4 + x
    onward = {"z": lax.rem(z + 7 + 2 * c, 8)}
    sibling = {"c": 1 - c}
    partner = {"yl": 1 - yl}

    barrier = pltpu.get_barrier_semaphore()
    near = [{"z": lax.rem(z + 1, 8)}, {"z": lax.rem(z + 7, 8)}] + [{"yh": lax.rem(yh + o, 4)} for o in (1, 2, 3)]
    for o in range(1, 16):
        there = lax.rem(state * 2 + c + o, 16)
        near.append({"yl": there // 8, "x": lax.rem(there // 2, 4), "c": lax.rem(there, 2)})
    for device in near:
        pl.semaphore_signal(barrier, inc=1, device_id=device, device_id_type=pl.DeviceIdType.MESH)
    own = [
        pltpu.make_async_copy(env_ref.at[0], rows.at[0, 0, c], local_sem.at[0]),
        pltpu.make_async_copy(edge_ref, pairs, local_sem.at[1]),
        pltpu.make_async_copy(block_ref.at[0], stored.at[pl.ds(0, 4), c], local_sem.at[2]),
        pltpu.make_async_copy(site_ref.at[0], stored.at[pl.ds(4, 2), c], local_sem.at[3]),
        pltpu.make_async_copy(current_ref, now, local_sem.at[4]),
        pltpu.make_async_copy(weight_ref, weights, local_sem.at[5]),
    ]
    for copy in own:
        copy.start()

    own[1].wait()
    for p in (0, 1):
        edges[0, 0, c, :, 256 * p:256 * (p + 1)] = pairs[:, p, :]
    pl.semaphore_wait(barrier, len(near))

    swap = [
        remote(block_ref.at[0], stored.at[pl.ds(0, 4), c], sent, s_recv, sibling),
        remote(site_ref.at[0], stored.at[pl.ds(4, 2), c], sent, s_recv, sibling),
    ]

    def passing(s, q, other):
        core = 1 - c if other else c
        return remote(rows.at[s, q, core], rows.at[s + 1, q, core], sent, z_recv.at[s, q, other], onward)

    def give(q):
        return remote(rows.at[0, 0, c], rows.at[0, q, c], sent, y_recv.at[q], {"yh": lax.rem(yh + 4 - q, 4)})

    def give_far(q):
        half = pl.ds(0 if q == 1 else 16, 16)
        return remote(rows.at[0, q, c, half], rows.at[0, 2, c, half], sent, y_recv.at[0 if q == 1 else 2],
                      {"yh": lax.rem(yh + 4 - q, 4)})

    def across(q):
        here = rows.at[0, q, c]
        return remote(here, here, sent, d_recv.at[q], sibling)

    def edge_of(s, place):
        return edges.at[s, place]

    edge_across = remote(edges.at[0, 0, c], edges.at[0, 0, c], sent, ed_recv, sibling)

    def edge_on(s):
        return remote(edges.at[s, 0], edges.at[s + 1, 0], sent, ez_recv.at[s], onward)

    def edge_side(s, q):
        return remote(edge_of(s, 0), edge_of(s, q), sent, ey_recv.at[s, 0], {"yh": lax.rem(yh + 4 - q, 4)})

    def edge_far(s):
        q = 1 + 2 * lax.rem(c + s, 2) if s in (1, 2, 3) else 3
        return remote(edge_of(s, q), edge_of(s, 2), sent, ey_recv.at[s, 1], {"yh": lax.rem(yh + 4 - q, 4)})

    def edge_spread(s):
        def side(q, core):
            @pl.when(jnp.logical_or(s in (1, 2, 3), c == core))
            def _():
                edge_side(s, q).start()

        side(1, 1)
        side(3, 0)

    def edge_relay(s):
        if s in (1, 2, 3):
            both = edges.at[s, pl.ds(0, 2)]
            pltpu.make_async_copy(both, both, ey_recv.at[s, 0]).wait()
            edge_far(s).start()
        else:
            @pl.when(c == 0)
            def _():
                edge_side(s, 3).wait_recv()
                edge_far(s).start()

    def edge_last(s):
        if s in (1, 2, 3):
            edge_far(s).wait_recv()
        else:
            @pl.when(c == 1)
            def _():
                edge_side(s, 1).wait_recv()

            @pl.when(c == 0)
            def _():
                edge_far(s).wait_recv()

    def edge_hop(s):
        edge_on(s - 1).wait_recv()
        if s < 4:
            edge_on(s).start()

    own[0].wait()
    passing(0, 0, 0).start()
    across(0).start()
    for q in (1, 3):
        give(q).start()
    edge_across.start()
    across(0).wait_recv()
    passing(0, 0, 1).start()
    edge_across.wait_recv()
    edge_on(0).start()

    own[4].wait()
    low, high = (now[:, :, 128 * h:128 * (h + 1)].astype(F32).reshape(128, 128) for h in (0, 1))
    current = turned(low, high, yh)
    grown[...] = jnp.zeros_like(grown)

    def origin(u):
        s = UNITS[u][0]
        return lax.rem(z + 8 + s - 2 * s * c, 8)

    def to_state(u, other, at_home=False):
        r = origin(u)
        core = 1 - c if other else c
        s, pair = UNITS[u]
        cut = pl.ds(128 * pair, 128) if s in (1, 2, 3) else pl.ds(pl.multiple_of(128 * (1 - c), 128), 128)
        there = proj_in.at[state, :, cut]
        if at_home:
            return pltpu.make_async_copy(proj_out.at[u, core], there, p_recv)
        return remote(proj_out.at[u, core], there, sent, p_recv,
                      {"yl": r // 4, "x": lax.rem(r, 4), "c": core})

    def moved_copy(s, other, device, sem):
        block = moved.at[s, (1 - yl if other else yl) * 4 + x]
        return remote(block, block, sent, m_recv.at[s, sem], device)

    def along_x(s, other, steps=(1, 2, 3)):
        return [near_x(s, other, o) for o in steps]

    def near_x(s, other, o):
        return moved_copy(s, other, {"x": lax.rem(x + o, 4)}, 1 if o == (3 if other else 1) else 2)

    def far_along_x(s, other):
        step = 3 if other else 1
        block = moved.at[s, (1 - yl if other else yl) * 4 + lax.rem(x + 4 - step, 4)]
        return remote(block, block, sent, m_recv.at[s, 2], {"x": lax.rem(x + step, 4)})

    def send_moved(s):
        moved_copy(s, False, partner, 0).start()
        for copy in along_x(s, False, (1, 3)):
            copy.start()
        if s == 7:
            @pl.when(c == 0)
            def _():
                near_x(s, False, 2).start()

    def send_proj(s):
        home = origin(s) == state

        @pl.when(home)
        def _():
            to_state(s, 0, True).start()

        @pl.when(jnp.logical_not(home))
        def _():
            to_state(s, 0).start()

        to_state(s, 1).start()

    def unit_of(ref, u):
        s, pair = UNITS[u]
        return ref.at[s, pl.ds(2 * pair if s in (1, 2, 3) else 2 * (1 - c), 2)]

    def product(u, start, stop):
        left = stored[start:stop].reshape(64 * (stop - start), WIDE)
        right = unit_of(rows, u)[...].reshape(128, WIDE)
        return lax.dot_general(left, right, (((1,), (1,)), ((), ())), preferred_element_type=F32).astype(BF)

    def keep_proj(u, value):
        blocks = value.reshape(4, 2, 32, 128)
        for j in (0, 1):
            proj_out[u, j] = blocks[:, j].reshape(128, 128)

    def multiply(u):
        if u == 7:
            moved[u, state] = product(u, 4, 6)
            send_moved(u)
            keep_proj(u, product(u, 0, 4))
            send_proj(u)
        else:
            both = product(u, 0, 6)
            keep_proj(u, both[0:256])
            moved[u, state] = both[256:384]
            send_moved(u)
            send_proj(u)

    def moved_here(s, count, sem):
        blocks = moved.at[s, pl.ds(0, count)]
        pltpu.make_async_copy(blocks, blocks, m_recv.at[s, sem]).wait()

    def relay(s):
        moved_copy(s, False, partner, 0).wait_recv()
        for copy in along_x(s, True, (1, 3)):
            copy.start()
        if s == 7:
            @pl.when(c == 0)
            def _():
                near_x(s, True, 2).start()

    def relay_far(s):
        moved_here(s, 2, 1)
        far_along_x(s, False).start()
        far_along_x(s, True).start()

    seen = set()

    def grow(u):
        s = UNITS[u][0]
        if s not in seen:
            seen.add(s)
            edge_last(s)
        if u == 7:
            @pl.when(c == 0)
            def _():
                moved_here(u, 2, 1)

        moved_here(u, 4, 2)
        site = unit_of(edges, u)[...].reshape(128, SITE)
        for p in (0, 1):
            right = moved[u, :, 64 * p:64 * (p + 1), :].reshape(512, 128)
            grown[...] += lax.dot_general(site[:, 256 * p:256 * (p + 1)], right, (((0,), (1,)), ((), ())),
                                          preferred_element_type=F32)

    def tasks(place):
        for task, u in TASKS.get(place, ()):
            (multiply, relay, relay_far, grow)[task](u)

    def last_chunks(core, chunks):
        @pl.when(c == core)
        def _():
            for q in chunks:
                for other in (0, 1):
                    passing(3, q, other).wait_recv()

    def last_row(core):
        @pl.when(c == core)
        def _():
            multiply(7)

    for place, (s, q) in enumerate(ORDER):
        if (s, q) == (0, 1):
            for near_q in (1, 3):
                give(near_q).wait_recv()
                give_far(near_q).start()
                across(near_q).start()
        if (s, q) == (0, 3):
            for near_q in (1, 3):
                give_far(near_q).wait_recv()
            across(2).start()
        if s == 0 and q:
            passing(0, q, 0).start()
            across(q).wait_recv()
            passing(0, q, 1).start()
        if s:
            for other in (0, 1):
                passing(s - 1, q, other).wait_recv()

                @pl.when(jnp.logical_or(s < 3, c == (1 if q < 2 else 0)))
                def _():
                    passing(s, q, other).start()
        if place == 1:
            for copy in swap:
                copy.start()
        if place == 4:
            own[2].wait()
            own[3].wait()
            pltpu.make_async_copy(stored.at[:, c], stored.at[:, c], s_recv).wait()
        for core, spots in ((1, (4, 8, 11)), (0, (8, 11, 13))):
            if place in spots:
                @pl.when(c == core)
                def _():
                    (multiply, relay, relay_far)[spots.index(place)](0)
        if place == 12:
            last_chunks(1, (0, 1))
            last_row(1)
        tasks(place)
        if place == 15:
            @pl.when(c == 1)
            def _():
                relay(7)
        if place in HOPS:
            edge_hop(HOPS[place])
        for t in SPREADS.get(place, ()):
            edge_spread(t)
        for t in RELAYS.get(place, ()):
            edge_relay(t)
    tasks(16)
    last_chunks(0, (3,))
    relay(6)
    tasks(17)

    @pl.when(c == 1)
    def _():
        relay_far(7)

    last_chunks(0, (2,))
    last_row(0)
    relay_far(5)
    tasks(19)

    @pl.when(c == 0)
    def _():
        relay(7)

    relay_far(6)
    for u in (3, 4, 5):
        grow(u)

    pltpu.make_async_copy(proj_in, proj_in, p_recv).wait()

    def projected(k, i):
        return proj_in[k, :, 128 * i:128 * (i + 1)].astype(F32)

    partial = [
        sum(jnp.sum((projected(k, i) * current[i]).reshape(16, 8, 128), axis=0) for i in (0, 1))
        for k in range(8)
    ]
    across_lanes = lax.broadcasted_iota(jnp.int32, (1, 128), 1)
    partial = sum(
        jnp.where(across_lanes == k, jnp.sum(jnp.sum(p, axis=0, keepdims=True), axis=1, keepdims=True), 0.0)
        for k, p in enumerate(partial)
    )

    places = (state * 2 + c, z * 4 + yh)
    sizes = (16, 32)

    def peer(stage, o):
        there = lax.rem(places[stage] + o, sizes[stage])
        if stage == 0:
            return {"yl": there // 8, "x": lax.rem(there // 2, 4), "c": lax.rem(there, 2)}
        return {"z": there // 4, "yh": lax.rem(there, 4)}

    def exchange(stage, value):
        dots[stage, places[stage]] = value
        for o in range(1, sizes[stage]):
            here = dots.at[stage, places[stage]]
            remote(here, here, sent, r_recv.at[stage], peer(stage, o)).start()

    def collected(stage):
        others = dots.at[stage, pl.ds(0, sizes[stage] - 1)]
        pltpu.make_async_copy(others, others, r_recv.at[stage]).wait()
        return jnp.sum(dots[stage, 0:sizes[stage]], axis=0)

    exchange(0, partial)
    grow(6)
    grow(7)
    give_half = remote(grown.at[pl.ds(128 * (1 - c), 128)], grown_in, sent, g_recv, sibling)
    give_half.start()
    give_half.wait_recv()

    lane = lax.broadcasted_iota(jnp.int32, (16, 128), 1)
    half = grown.at[pl.ds(pl.multiple_of(128 * c, 128), 128)]
    for d in range(4):
        for pair in range(4):
            cut = pl.ds(128 * pair, 128)
            first = half[pl.ds(32 * d, 16), cut] + grown_in[pl.ds(32 * d, 16), cut]
            second = half[pl.ds(32 * d + 16, 16), cut] + grown_in[pl.ds(32 * d + 16, 16), cut]
            tiles_out[2 * pair, d] = jnp.where(lane < 64, first, pltpu.roll(second, 64, 1)).astype(BF)
            tiles_out[2 * pair + 1, d] = jnp.where(lane < 64, pltpu.roll(first, 64, 1), second).astype(BF)

    place = z * 4 + yh
    for k in range(8):
        for d in range(4):
            to = 2 * c + d // 2
            here = jnp.logical_and(jnp.logical_and(k == state, z == state), jnp.logical_and(to == yh, d % 2 == c))

            @pl.when(here)
            def _():
                pltpu.make_async_copy(tiles_out.at[k, d], tiles_in.at[place], o_recv).start()

            @pl.when(jnp.logical_not(here))
            def _():
                remote(tiles_out.at[k, d], tiles_in.at[place], sent, o_recv,
                       {"yl": k // 4, "x": k % 4, "z": state, "yh": to, "c": d % 2}).start()

    exchange(1, collected(0))
    own[5].wait()
    total = collected(1) * (1.0 / 4096.0)
    factor = [total[:, k:k + 1] * weights[k] for k in range(8)]
    halves = []
    for i in (0, 1):
        value = current[i]
        for k in range(8):
            value = value + factor[k] * projected(k, i)
        halves.append(value)
    low, high = turned(*halves, lax.rem(4 - yh, 4))
    pen_out[:, :, 0:128] = low.reshape(4, 32, 128)
    pen_out[:, :, 128:256] = high.reshape(4, 32, 128)

    pen_copy = pltpu.make_async_copy(pen_out, pen_ref, local_sem.at[1])
    pen_copy.start()

    pltpu.make_async_copy(tiles_in, tiles_in, o_recv).wait()
    for p in range(16):
        even = tiles_in[2 * p].astype(F32)
        odd = tiles_in[2 * p + 1].astype(F32)
        cut = slice(128 * p, 128 * (p + 1))
        next_out[ 0:16, cut] = jnp.where(lane < 64, even, pltpu.roll(odd, 64, 1)).astype(BF)
        next_out[ 16:32, cut] = jnp.where(lane < 64, pltpu.roll(even, 64, 1), odd).astype(BF)

    next_copy = pltpu.make_async_copy(next_out, next_ref.at[0], local_sem.at[0])
    next_copy.start()

    def drained(ref, sem):
        pltpu.make_async_copy(ref, ref, sem).wait()

    drained(stored.at[:, c], sent)
    drained(rows.at[0, pl.ds(0, 3), 0], sent)
    drained(rows.at[0, :, 0], sent)
    drained(rows.at[pl.ds(0, 3)], sent)
    drained(rows.at[3, :, 0], sent)
    drained(edges.at[pl.ds(0, 3)], sent)
    drained(edges.at[3, pl.ds(0, 3)], sent)
    drained(edges.at[3, 3, 0], sent)

    @pl.when(c == 0)
    def _():
        drained(edges.at[0, pl.ds(0, 2)], sent)

    for t in range(8):
        @pl.when(origin(t) != state)
        def _():
            drained(proj_out.at[0, 0], sent)

    drained(proj_out.at[pl.ds(0, 4)], sent)
    drained(moved.at[pl.ds(0, 7)], sent)
    drained(grown_in, sent)
    for stage in range(2):
        drained(dots.at[stage, pl.ds(0, sizes[stage] - 1)], sent)
    drained(tiles_in.at[pl.ds(0, 31)], sent)

    @pl.when(jnp.logical_not(jnp.logical_and(z == state, yh // 2 == c)))
    def _():
        drained(tiles_in.at[0], sent)
    next_copy.wait()
    pen_copy.wait()


def shards(intersect_left, stored_block, stored_site, current_site, current_block, penalty_weight):
    hbm = pl.BlockSpec(memory_space=pl.ANY)
    dma = pltpu.SemaphoreType.DMA
    return pl.pallas_call(
        kernel,
        out_shape=(
            jax.ShapeDtypeStruct((4, 32, 256), F32),
            jax.ShapeDtypeStruct((1, 32, 2048), BF),
        ),
        in_specs=[hbm] * 6,
        out_specs=(hbm, hbm),
        scratch_shapes=[
            pltpu.VMEM((5, 4, 2, 32, WIDE), BF),
            pltpu.VMEM((6, 2, 32, WIDE), BF),
            pltpu.VMEM((5, 4, 2, 32, SITE), BF),
            pltpu.VMEM((4, 32, 256), BF),
            pltpu.VMEM((8, 2, 128, 128), BF),
            pltpu.VMEM((8, 128, 256), BF),
            pltpu.VMEM((8, 8, 128, 128), BF),
            pltpu.VMEM((256, 512), F32),
            pltpu.VMEM((128, 512), F32),
            pltpu.VMEM((8, 4, 16, 128), BF),
            pltpu.VMEM((32, 16, 128), BF),
            pltpu.VMEM((2, 32, 1, 128), F32),
            pltpu.SMEM((8,), F32),
            pltpu.VMEM((4, 32, 256), F32),
            pltpu.VMEM((32, 2048), BF),
            pltpu.VMEM((32, 2, 256), BF),
            dma((6,)), dma, dma((4,)), dma((4,)), dma((4, 4, 2)), dma, dma, dma((8, 3)), dma, dma, dma((2,)),
            dma, dma((4,)), dma((5, 2)),
        ],
        compiler_params=pltpu.CompilerParams(collective_id=0, has_side_effects=True, vmem_limit_bytes=63 * 1024 * 1024),
        name="project_and_grow",
    )(intersect_left, stored_block, stored_site, current_site, current_block, penalty_weight)


def solution(mesh):
    torus = Mesh(mesh.devices.reshape(2, 4, 8, 4, 2), STATE + BOND)
    in_specs = (
        P(STATE, BOND, None),
        P(STATE, None, BOND, None),
        P(STATE, None, BOND, None),
        P(BOND, None, STATE),
        P(None, BOND, STATE),
        P(),
    )
    out_specs = (P(None, BOND, STATE), P(STATE, BOND, None))
    return jax.shard_map(shards, mesh=torus, in_specs=in_specs, out_specs=out_specs, check_vma=False)
```
